32 devices in a mesh: dp: 8 (over z, y), tensor: 4 (over x, core).
Axes of the slice: x: 2, y: 2, z: 4, core: 2. Of those that a mesh axis runs over, the one named last changes fastest.
Arguments:
- hidden_in: bfloat16 [256, 4096], P('dp'), may hold values from -6 to 6
- norm_gain: float32 [4096], replicated, may hold values from 0.5 to 1.5
- w_in: bfloat16 [4096, 2, 4, 2048], P(None, None, 'tensor', 'dp'), may hold values from -0.09375 to 0.09375
- conv_w: float32 [4, 8192], P(None, 'tensor'), may hold values from -3 to 3
- conv_b: float32 [8192], P('tensor'), may hold values from -2 to 2
- w_dt_low: bfloat16 [8192, 256], P('tensor'), may hold values from -0.0625 to 0.0625
- w_bc: bfloat16 [32, 8192], P(None, 'tensor'), may hold values from -0.0625 to 0.0625
- w_dt: bfloat16 [256, 8192], P(None, 'tensor'), may hold values from -0.375 to 0.375
- dt_bias: float32 [8192], P('tensor'), may hold values from -5 to -1.5
- a_log: float32 [16, 8192], P(None, 'tensor'), may hold values from 0 to 2.77
- d_skip: float32 [8192], P('tensor'), may hold values from 0.5 to 1.5
- w_out: bfloat16 [8192, 4096], P('tensor', 'dp'), may hold values from -0.0625 to 0.0625
- conv_state: bfloat16 [256, 3, 8192], P('dp', None, 'tensor'), may hold values from -6 to 6
- ssm_state: float32 [256, 16, 8192], P('dp', None, 'tensor'), may hold values from -6 to 6
- lengths: int32 [256], P('dp'), may hold values from 0 to 5
- active_ids: int32 [8, 32], P('dp'), may hold values from 0 to 31, each once within a row
- active_count: int32 [8], P('dp'), may hold values from 1 to 24, as said below
Outputs:
- mixed: bfloat16 [256, 4096], P('dp', 'tensor')
- conv_next: bfloat16 [256, 3, 8192], P('dp', None, 'tensor')
- ssm_next: float32 [256, 16, 8192], P('dp', None, 'tensor')
The draws below stay inside these ranges and needn't reach their ends.
Inputs may be any that keep to these rules, and one draw needn't show every extreme that they name: `active_count`: at most 24 slots of a dp index are active; some dp index has exactly 24. `active_ids`: each row lists every slot 0 to 31 of its dp index once.
All inputs are finite; a program needn't handle non-finite values.
Results may differ from the reference program's by a relative error of at most 0.014.
Values may be sent and summed in bfloat16 or wider, within the bound.
No kernel may reach another device: no remote copies, remote signals or barrier semaphores. Data moves between devices by JAX's collectives and lax.ppermute only.
A program may use at most 128 MiB of HBM per device.

```python
import jax
import jax.numpy as jnp
from jax import lax

D = 4096
E = 8192
N = 16
R = 256
K = 4
SEQ_DEV = 32
ACT_MAX = 24
BATCH = 256
N_DP = 8
N_TENSOR = 4


def draw_active_count(key, part):
    first, second, third = jax.random.split(jax.random.fold_in(key, 17), 3)
    one_draw = jax.random.randint(first, (N_DP,), 1, ACT_MAX + 1)
    two_draw = jax.random.randint(second, (N_DP,), 1, ACT_MAX + 1)
    skewed = jnp.minimum(one_draw, two_draw)
    chosen = jax.random.randint(third, (), 0, N_DP)
    return skewed.at[chosen].set(ACT_MAX).astype(jnp.int32)


def set_ends(entries, stream_key, least, top_value):
    shape = entries.shape
    index_at = [jax.random.randint(jax.random.fold_in(stream_key, axis), (), 0, shape[axis]) for axis in range(len(shape))]
    entries = entries.at[tuple(index_at)].set(least)
    longest = shape.index(max(shape))
    index_at[longest] = (index_at[longest] + 1) % shape[longest]
    return entries.at[tuple(index_at)].set(top_value)


def levels(rng, extent, cuts, low, largest):
    factor_of = 1.0
    for dim, shards_of in cuts:
        draws = jax.random.uniform(jax.random.fold_in(jax.random.fold_in(rng, 6), dim), (shards_of,), jnp.float32, low / len(cuts), largest / len(cuts))
        factor_of = factor_of * jnp.repeat(jnp.exp(draws), extent[dim] // shards_of).reshape((-1,) + (1,) * (len(extent) - 1 - dim))
    return factor_of


def scatter_about(own_key, shape, width, bound, cuts=(), kind=jnp.bfloat16):
    values = jax.random.normal(own_key, shape, jnp.float32) * width
    if len(cuts) > 0:
        values = levels(own_key, shape, cuts, -0.22, 0.18) * values
    return jnp.clip(values, min=-bound, max=bound).astype(kind)


def setup_inputs(seed: int = 0) -> dict:
    arg_keys = jax.random.split(jax.random.key(seed), 18)
    hidden_in = scatter_about(arg_keys[0], (BATCH, D), 1.0, 6.0, ((0, 8),))
    norm_gain = jnp.clip(1.0 + 0.1 * jax.random.normal(arg_keys[1], (D,), jnp.float32), 0.5, 1.5)
    w_in = scatter_about(arg_keys[2], (D, 2, N_TENSOR, E // N_TENSOR), D ** -0.5, 0.09375, ((2, 4), (3, 8)))
    conv_w = scatter_about(arg_keys[3], (K, E), 0.5, 3.0, ((1, 4),), jnp.float32)
    conv_b = scatter_about(arg_keys[4], (E,), 0.3, 2.0, ((0, 4),), jnp.float32)
    w_dt_low = scatter_about(arg_keys[5], (E, R), E ** -0.5, 0.0625, ((0, 4),))
    w_bc = scatter_about(arg_keys[6], (2 * N, E), E ** -0.5, 0.0625, ((1, 4),))
    w_dt = scatter_about(arg_keys[7], (R, E), R ** -0.5, 0.375, ((1, 4),))
    dt_bias = jnp.clip(-5.0 + 3.5 * jax.random.uniform(arg_keys[8], (E,), jnp.float32) ** levels(arg_keys[8], (E,), ((0, 4),), -0.2, 0.2), -5.0, -1.5)
    a_log = jnp.clip(2.77 * jax.random.uniform(arg_keys[9], (N, E), jnp.float32) ** levels(arg_keys[9], (N, E), ((1, 4),), -0.2, 0.2), 0.0, 2.77)
    d_skip = jnp.clip(0.5 + 1.0 * jax.random.uniform(arg_keys[10], (E,), jnp.float32) ** levels(arg_keys[10], (E,), ((0, 4),), -0.2, 0.2), 0.5, 1.5)
    w_out = scatter_about(arg_keys[11], (E, D), E ** -0.5, 0.0625, ((0, 4), (1, 8)))
    conv_state = scatter_about(arg_keys[12], (BATCH, K - 1, E), 1.0, 6.0, ((0, 8), (2, 4)))
    ssm_state = scatter_about(arg_keys[13], (BATCH, N, E), 1.0, 6.0, ((0, 8), (2, 4)), jnp.float32)
    lengths = set_ends(jax.random.randint(arg_keys[14], (BATCH,), 0, 6), jax.random.fold_in(arg_keys[14], 1), 0, 5).astype(jnp.int32)
    active_ids = jax.vmap(lambda own: jax.random.permutation(own, SEQ_DEV))(jax.random.split(arg_keys[15], N_DP)).reshape((N_DP, SEQ_DEV)).astype(jnp.int32)
    active_count = draw_active_count(jax.random.fold_in(arg_keys[17], 71), 0)
    return dict(hidden_in=hidden_in, norm_gain=norm_gain, w_in=w_in, conv_w=conv_w, conv_b=conv_b, w_dt_low=w_dt_low, w_bc=w_bc, w_dt=w_dt, dt_bias=dt_bias, a_log=a_log, d_skip=d_skip, w_out=w_out, conv_state=conv_state, ssm_state=ssm_state, lengths=lengths, active_ids=active_ids, active_count=active_count)


def rms_rows(values, epsilon):
    return values * lax.rsqrt(lax.optimization_barrier(jnp.mean(values * values, axis=-1, keepdims=True)) + epsilon)

def active_slots(active_ids, active_count):
    order = jnp.arange(active_ids.shape[-1], dtype=jnp.int32)
    early = order[None, :] < active_count[:, None]
    hits = (active_ids[:, :, None] == order[None, None, :]) & early[:, :, None]
    return jnp.any(hits, axis=1)

def filter_step(conv_state, x_in, lengths, conv_w, conv_b):
    window = jnp.concatenate([conv_state, x_in[:, None, :]], axis=1)
    taps = window.shape[1]
    offsets = jnp.arange(taps, dtype=jnp.int32)
    usable = (lengths[:, None] - (taps - 1) + offsets[None, :] >= 0).astype(jnp.float32)
    summed = lax.optimization_barrier(jnp.sum(window.astype(jnp.float32) * conv_w[None] * usable[:, :, None], axis=1)) + conv_b
    return (window, jax.nn.silu(summed).astype(jnp.bfloat16))

def projections(filtered, w_dt_low, w_bc):
    low = jnp.dot(filtered, w_dt_low, preferred_element_type=jnp.float32)
    both = lax.dot_general(filtered, w_bc, (((1,), (1,)), ((), ())), preferred_element_type=jnp.float32)
    return (low, both)

def step_sizes(low, w_dt, dt_bias):
    low_normed = rms_rows(low, 1e-06).astype(jnp.bfloat16)
    return jax.nn.softplus(jnp.dot(low_normed, w_dt, preferred_element_type=jnp.float32) + dt_bias)

def state_update(state, step_size, b_in, c_out, filtered, z_in, fresh, a_log, d_skip):
    filt_f = filtered.astype(jnp.float32)
    factor = jnp.exp(-step_size[:, None, :] * jnp.exp(a_log)[None])
    updated = factor * state * fresh[:, None, None] + step_size[:, None, :] * b_in[:, :, None] * filt_f[:, None, :]
    output = lax.optimization_barrier(jnp.sum(c_out[:, :, None] * updated, axis=1)) + d_skip * filt_f
    gated = output * jax.nn.silu(z_in.astype(jnp.float32))
    return (updated, gated.astype(jnp.bfloat16))

def reference(hidden_in, norm_gain, w_in, conv_w, conv_b, w_dt_low, w_bc, w_dt, dt_bias, a_log, d_skip, w_out, conv_state, ssm_state, lengths, active_ids, active_count):
    active = active_slots(active_ids, active_count).reshape(-1)
    hidden_f = hidden_in.astype(jnp.float32)
    normed = (rms_rows(hidden_f, 1e-05) * norm_gain).astype(jnp.bfloat16)
    w_flat = w_in.reshape(D, 2, E)
    x_in = jnp.dot(normed, w_flat[:, 0], preferred_element_type=jnp.float32).astype(jnp.bfloat16)
    z_in = jnp.dot(normed, w_flat[:, 1], preferred_element_type=jnp.float32).astype(jnp.bfloat16)
    window, filtered = filter_step(conv_state, x_in, lengths, conv_w, conv_b)
    low, both = projections(filtered, w_dt_low, w_bc)
    b_normed = rms_rows(both[:, :N], 1e-06)
    c_normed = rms_rows(both[:, N:], 1e-06)
    step_size = step_sizes(low, w_dt, dt_bias)
    fresh = (lengths > 0).astype(jnp.float32)

    def grouped(values):
        return values.reshape((N_DP, SEQ_DEV) + values.shape[1:])

    def per_group(items):
        return state_update(*items, a_log, d_skip)
    updated, gated = lax.map(per_group, (grouped(ssm_state), grouped(step_size), grouped(b_normed), grouped(c_normed), grouped(filtered), grouped(z_in), grouped(fresh)))
    updated = updated.reshape(ssm_state.shape)
    gated = gated.reshape(BATCH, E)
    projected = jnp.dot(gated, w_out, preferred_element_type=jnp.float32)
    mixed = (hidden_f + active.astype(jnp.float32)[:, None] * projected).astype(jnp.bfloat16)
    conv_next = jnp.where(active[:, None, None], window[:, 1:], conv_state)
    ssm_next = jnp.where(active[:, None, None], updated, ssm_state)
    return (mixed, conv_next, ssm_next)
```

```python
import jax
import jax.numpy as jnp
from jax import lax
from jax.sharding import PartitionSpec as P

ACT_MAX = 24


def rms_rows(values, epsilon):
    return values * lax.rsqrt(jnp.mean(values * values, axis=-1, keepdims=True) + epsilon)


def swap_by(values, axis, size, mask):
    return lax.ppermute(values, axis, [(i, i ^ mask) for i in range(size)])


def gather_blocks(block, n_dp):
    far, near, side = (swap_by(block, "dp", n_dp, m) for m in (4, 2, 1))
    cross = swap_by(block, "dp", n_dp, 6)
    near_s, far_s, cross_s = (swap_by(b, "dp", n_dp, 1) for b in (near, far, cross))
    return [block, side, near, near_s, far, far_s, cross, cross_s]


def sum_tensor(values, n_t):
    total = values
    for mask in range(1, n_t):
        total = total + swap_by(values, "tensor", n_t, mask)
    return total


def filter_step(conv_state, x_in, lengths, conv_w, conv_b):
    window = jnp.concatenate([conv_state, x_in[:, None, :]], axis=1)
    taps = window.shape[1]
    offsets = jnp.arange(taps, dtype=jnp.int32)
    usable = (lengths[:, None] - (taps - 1) + offsets[None, :] >= 0).astype(jnp.float32)
    summed = (
        jnp.sum(window.astype(jnp.float32) * conv_w[None] * usable[:, :, None], axis=1) + conv_b
    )
    return (window, jax.nn.silu(summed).astype(jnp.bfloat16))


def state_update(state, step_size, b_in, c_out, filtered, z_in, fresh, a_log, d_skip):
    filt_f = filtered.astype(jnp.float32)
    factor = jnp.exp(-step_size[:, None, :] * jnp.exp(a_log)[None])
    updated = (
        factor * state * fresh[:, None, None]
        + step_size[:, None, :] * b_in[:, :, None] * filt_f[:, None, :]
    )
    output = jnp.sum(c_out[:, :, None] * updated, axis=1) + d_skip * filt_f
    gated = output * jax.nn.silu(z_in.astype(jnp.float32))
    return (updated, gated.astype(jnp.bfloat16))


def make_body(n_dp, n_t):
    direct = n_dp == 8 and n_t == 4

    def body(
        hidden_in,
        norm_gain,
        w_in,
        conv_w,
        conv_b,
        w_dt_low,
        w_bc,
        w_dt,
        dt_bias,
        a_log,
        d_skip,
        w_out,
        conv_state,
        ssm_state,
        lengths,
        active_ids,
        active_count,
    ):
        f32, bf16 = jnp.float32, jnp.bfloat16
        slots = hidden_in.shape[0]
        rows = min(ACT_MAX, slots)
        g = lax.axis_index("dp")
        t = lax.axis_index("tensor")
        ids = active_ids[0, :rows]
        pick = ids[:, None] == jnp.arange(slots, dtype=jnp.int32)[None, :]
        pick_b = pick.astype(bf16)
        early = jnp.arange(rows, dtype=jnp.int32) < active_count[0]
        flagged = jnp.any(pick & early[:, None], axis=0)

        def compact(v):
            return jnp.dot(pick_b, v, preferred_element_type=f32).astype(bf16)

        def spread(v):
            return lax.dot_general(
                pick_b, v, (((0,), (0,)), ((), ())), preferred_element_type=f32
            ).astype(bf16)

        chosen = compact(hidden_in).astype(f32)
        normed = (rms_rows(chosen, 1e-05) * norm_gain).astype(bf16)
        depth = w_in.shape[0]
        width_block = w_in.shape[3]
        w_local = w_in.reshape(depth, 2 * width_block)
        if direct:
            core = t % 2
            half = depth // 2
            mine = gather_blocks(lax.dynamic_slice_in_dim(normed, core * half, half, 1), n_dp)
            other = [swap_by(b, "tensor", n_t, 1) for b in mine]
            mine, other = jnp.stack(mine), jnp.stack(other)
            first = jnp.where(core == 0, mine, other)
            second = jnp.where(core == 0, other, mine)
            full = jnp.concatenate([first, second], axis=2).reshape(n_dp * rows, depth)
        else:
            full = lax.all_gather(normed, "dp", axis=0, tiled=True)
        branches = jnp.dot(full, w_local, preferred_element_type=f32).astype(bf16)
        if direct:
            order = jnp.arange(n_dp, dtype=jnp.int32) ^ g
            branches = jnp.take(branches.reshape(n_dp, rows, -1), order, axis=0)
            branches = branches.reshape(n_dp * rows, -1)
        owned = lax.all_to_all(branches, "dp", split_axis=0, concat_axis=0, tiled=True)
        owned = owned.reshape(n_dp, rows, 2, width_block)
        x_c = jnp.transpose(owned[:, :, 0], (1, 0, 2)).reshape(rows, n_dp * width_block)
        z_c = jnp.transpose(owned[:, :, 1], (1, 0, 2)).reshape(rows, n_dp * width_block)
        x_in, z_in = spread(x_c), spread(z_c)
        window, filtered = filter_step(conv_state, x_in, lengths, conv_w, conv_b)
        low = jnp.dot(filtered, w_dt_low, preferred_element_type=f32)
        both = lax.dot_general(filtered, w_bc, (((1,), (1,)), ((), ())), preferred_element_type=f32)
        packed = jnp.concatenate([low, both], axis=1)
        packed = sum_tensor(packed, n_t) if direct else lax.psum(packed, "tensor")
        low, both = packed[:, : low.shape[1]], packed[:, low.shape[1] :]
        low_normed = rms_rows(low, 1e-06).astype(bf16)
        step_size = jax.nn.softplus(
            jnp.dot(low_normed, w_dt, preferred_element_type=f32) + dt_bias
        )
        fresh = (lengths > 0).astype(f32)
        state_count = w_bc.shape[0] // 2
        b_normed = rms_rows(both[:, :state_count], 1e-06)
        c_normed = rms_rows(both[:, state_count:], 1e-06)
        updated, gated = state_update(
            ssm_state, step_size, b_normed, c_normed, filtered, z_in, fresh, a_log, d_skip
        )
        gated_c = compact(gated)
        share = hidden_in.shape[1] // n_t
        if direct:
            blocks = jnp.concatenate(gather_blocks(gated_c, n_dp), axis=0)
            columns = jnp.dot(blocks, w_out, preferred_element_type=f32)
            columns = columns.reshape(n_dp, rows, -1)
            base = 2 * (t ^ 2)
            parts = []
            for m in range(n_t):
                pair = (base ^ (2 * m)) + jnp.arange(2, dtype=jnp.int32)
                parts.append(jnp.take(columns, pair ^ g, axis=0))
            total = parts[0]
            for m in range(1, n_t):
                total = total + swap_by(parts[m].astype(bf16), "tensor", n_t, m).astype(f32)
            total = total.astype(bf16)
            side = g % 2
            got = []
            for k in range(2):
                perm = []
                for gg in range(n_dp):
                    for tt in range(n_t):
                        dest = 2 * (tt ^ 2) + ((gg % 2) ^ k)
                        perm.append((gg * n_t + tt, dest * n_t + gg // 2))
                sent = lax.dynamic_index_in_dim(total, side ^ k, 0, keepdims=False)
                got.append(lax.ppermute(sent, ("dp", "tensor"), perm))
            left = jnp.where(side == 0, got[0], got[1])
            right = jnp.where(side == 0, got[1], got[0])
            projected = jnp.concatenate([left, right], axis=1)
        else:
            blocks = lax.all_gather(gated_c, "dp", axis=0, tiled=True)
            columns = jnp.dot(blocks, w_out, preferred_element_type=f32).astype(bf16)
            by_sequence = lax.all_to_all(columns, "dp", split_axis=0, concat_axis=1, tiled=True)
            projected = lax.psum_scatter(by_sequence, "tensor", scatter_dimension=1, tiled=True)
        hidden_cols = lax.dynamic_slice_in_dim(hidden_in, t * share, share, 1)
        flag_f = flagged.astype(f32)[:, None]
        mixed_part = (
            hidden_cols.astype(f32) + flag_f * spread(projected).astype(f32)
        ).astype(bf16)
        conv_part = jnp.where(flagged[:, None, None], window[:, 1:], conv_state)
        state_part = jnp.where(flagged[:, None, None], updated, ssm_state)
        return (mixed_part, conv_part, state_part)

    return body


def solution(mesh):
    in_specs = (
        P("dp", None),
        P(),
        P(None, None, "tensor", "dp"),
        P(None, "tensor"),
        P("tensor"),
        P("tensor", None),
        P(None, "tensor"),
        P(None, "tensor"),
        P("tensor"),
        P(None, "tensor"),
        P("tensor"),
        P("tensor", "dp"),
        P("dp", None, "tensor"),
        P("dp", None, "tensor"),
        P("dp"),
        P("dp", None),
        P("dp"),
    )
    out_specs = (P("dp", "tensor"), P("dp", None, "tensor"), P("dp", None, "tensor"))
    body = make_body(mesh.shape["dp"], mesh.shape["tensor"])
    return jax.shard_map(body, mesh=mesh, in_specs=in_specs, out_specs=out_specs, check_vma=False)
```

```python
import jax
import jax.numpy as jnp
from jax import lax
from jax.experimental import pallas as pl
from jax.experimental.pallas import tpu as pltpu
from jax.sharding import PartitionSpec as P

ACT_MAX = 24
TIE = 3


F32 = jnp.float32
BF16 = jnp.bfloat16
VMEM = pl.BlockSpec(memory_space=pltpu.VMEM)
SMEM = pl.BlockSpec(memory_space=pltpu.SMEM)
HBM = pl.BlockSpec(memory_space=pl.ANY)


def rms_rows(values, epsilon):
    return values * lax.rsqrt(jnp.mean(values * values, axis=-1, keepdims=True) + epsilon)


def silu(values):
    return values / (1.0 + jnp.exp(-values))


def iota(shape, dim):
    return lax.broadcasted_iota(jnp.int32, shape, dim)


def norm_kernel(ids, count, place, hidden, gain, chosen, pick, spread, columns):
    rows = chosen.shape[0]
    slots = hidden.shape[0]
    share = columns.shape[1]
    across = iota((rows, slots), 0), iota((rows, slots), 1)
    back = iota((slots, rows), 0), iota((slots, rows), 1)
    one_hot = jnp.zeros((rows, slots), F32)
    live = jnp.zeros((slots, rows), F32)
    for j in range(rows):
        slot = ids[0, j]
        early = jnp.where(j < count[0], 1.0, 0.0)
        one_hot = jnp.where((across[0] == j) & (across[1] == slot), 1.0, one_hot)
        live = jnp.where((back[1] == j) & (back[0] == slot), early, live)
    selected = one_hot.astype(BF16)
    pick[...] = selected
    spread[...] = live.astype(BF16)
    values = jnp.dot(selected, hidden[...], preferred_element_type=F32)
    chosen[...] = (rms_rows(values, 1e-05) * gain[...]).astype(BF16)
    columns[...] = hidden[:, pl.ds(pl.multiple_of(place[0] * share, 128), share)]


def filter_kernel(x_new, z_new, spread, lengths, conv_state, conv_w, conv_b, w_dt_low, w_bc,
                  packed, filtered, x_in, z_in):
    taps = conv_w.shape[0]
    width = conv_w.shape[1]

    def branch(ref, first):
        if len(ref.shape) == 2:
            return ref[...]
        block = ref.shape[2] // 2
        parts = [ref[k, :, first * block : (first + 1) * block] for k in range(ref.shape[0])]
        return jnp.concatenate(parts, axis=1)

    def to_slots(values):
        return jnp.dot(spread[...], values, preferred_element_type=F32)

    x_slots = to_slots(branch(x_new, 0))
    x_in[...] = x_slots.astype(BF16)
    known = lengths[...]
    total = conv_w[taps - 1 : taps, :] * x_slots * (known >= 0).astype(F32)
    for k in range(taps - 1):
        usable = (known >= taps - 1 - k).astype(F32)
        total = total + conv_w[k : k + 1, :] * conv_state[k].astype(F32) * usable
    result = silu(total + conv_b[...]).astype(BF16)
    filtered[...] = result
    rank = w_dt_low.shape[1]
    packed[:, :rank] = jnp.dot(result, w_dt_low[...], preferred_element_type=F32)
    packed[:, rank:] = lax.dot_general(
        result, w_bc[...], (((1,), (1,)), ((), ())), preferred_element_type=F32
    )
    z_in[...] = to_slots(branch(z_new, 1)).astype(BF16)


def state_kernel(*refs, parts, group, wide):
    sums = refs[:parts]
    (w_dt, dt_bias, a_log, d_skip, filtered, z_in, lengths, active, pick, states,
     gated, states_next,
     buffer, result, step, drive, b_wide, c_wide, decay, out, in_sem, out_sem) = refs[parts:]
    count = a_log.shape[0]
    slots, width = filtered.shape
    chunks = slots // group
    span = group * count

    def move(k, i, source, target, sem, out_of_hbm):
        piece = pl.ds(k * span, span)
        lanes = pl.ds(pl.multiple_of(i * 128, 128), 128)
        hbm, local = (source, target) if out_of_hbm else (target, source)
        ends = hbm.at[piece, lanes], local.at[i, piece]
        ends = ends if out_of_hbm else ends[::-1]
        return pltpu.make_async_copy(*ends, sem.at[k, i])

    def load(k, i):
        return move(k, i, states, buffer, in_sem, True)

    def save(k, i):
        return move(k, i, result, states_next, out_sem, False)

    tiles = width // 128
    for k in range(chunks):
        for i in range(tiles):
            load(k, i).start()
    total = sums[0][...]
    for other in sums[1:]:
        total = total + other[...]
    rank = w_dt.shape[0]
    low = rms_rows(total[:, :rank], 1e-06).astype(BF16)
    b_in = rms_rows(total[:, rank : rank + count], 1e-06)
    c_out = rms_rows(total[:, rank + count : rank + 2 * count], 1e-06)
    raw = jnp.dot(low, w_dt[...], preferred_element_type=F32) + dt_bias[...]
    size = jnp.maximum(raw, 0.0) + jnp.log1p(jnp.exp(-jnp.abs(raw)))
    step[...] = size
    drive[...] = size * filtered[...].astype(F32)
    decay[...] = -jnp.exp(a_log[...])
    for n in range(count):
        b_wide[n] = jnp.broadcast_to(b_in[:, n : n + 1], (slots, 128))
        c_wide[n] = jnp.broadcast_to(c_out[:, n : n + 1], (slots, 128))
    for k in range(chunks):
        rows = slice(k * group, (k + 1) * group)
        fresh = jnp.broadcast_to((lengths[rows, :] > 0).astype(F32), (group, 128))
        keep = jnp.broadcast_to(active[rows, :], (group, 128)) > 0.5

        def column(i, carry):
            tile = [i * wide + u for u in range(wide)]
            lanes = [pl.ds(pl.multiple_of(v * 128, 128), 128) for v in tile]
            for v in tile:
                load(k, v).wait()
            size = [step[rows, at] for at in lanes]
            push = [drive[rows, at] for at in lanes]
            y = [jnp.zeros((group, 128), F32) for _ in tile]
            for n in range(count):
                at = pl.ds(k * span + n, group, stride=count)
                b_n = b_wide[n, rows, :]
                c_n = c_wide[n, rows, :]
                for u in range(wide):
                    old = buffer[tile[u], at, :]
                    scale = jnp.exp(size[u] * decay[n : n + 1, lanes[u]])
                    new = scale * (old * fresh) + push[u] * b_n
                    y[u] = y[u] + c_n * new
                    result[tile[u], at, :] = jnp.where(keep, new, old)
            for u in range(wide):
                out[rows, lanes[u]] = y[u]
                save(k, tile[u]).start()
            return carry

        lax.fori_loop(0, tiles // wide, column, 0)
    filt = filtered[...].astype(F32)
    mixed = (out[...] + d_skip[...] * filt) * silu(z_in[...].astype(F32))
    gated[...] = jnp.dot(
        pick[...], mixed.astype(BF16), preferred_element_type=F32
    ).astype(BF16)
    for k in range(chunks):
        for i in range(tiles):
            save(k, i).wait()


def mix_kernel(spread, columns, first, second, mixed):
    half = first.shape[1]
    matrix = spread[...]
    for i, ref in enumerate((first, second)):
        lanes = slice(i * half, (i + 1) * half)
        added = jnp.dot(matrix, ref[...], preferred_element_type=F32)
        mixed[:, lanes] = (columns[:, lanes].astype(F32) + added).astype(BF16)


def swap_by(values, axis, size, mask):
    return lax.ppermute(values, axis, [(i, i ^ mask) for i in range(size)])


def swap_by_core(values, n_dp, n_t, masks):
    perm = []
    for g in range(n_dp):
        for t in range(n_t):
            perm.append(((g ^ masks[t % 2]) * n_t + t, g * n_t + t))
    return lax.ppermute(values, ("dp", "tensor"), perm)


def gather_shared(block, g, t, n_dp, n_t):
    even = t % 2 == 0
    side = swap_by_core(block, n_dp, n_t, (1, 1))
    far = swap_by_core(block, n_dp, n_t, (4, 2))
    far_side = swap_by_core(far, n_dp, n_t, (1, 1))
    last = swap_by_core(jnp.where(even, far, side), n_dp, n_t, (2, 6))
    swapped = [swap_by(v, "tensor", n_t, 1) for v in (far, far_side, last)]
    blocks = [block, side, far, far_side, last] + swapped
    masks = ((0, 0), (1, 1), (4, 2), (5, 3), (6, 7), (2, 4), (3, 5), (7, 6))
    return blocks, [g ^ jnp.where(even, a, b) for a, b in masks]


def gather_own(block, g, n_dp):
    far, near, side = (swap_by(block, "dp", n_dp, m) for m in (4, 2, 1))
    both = swap_by(far, "dp", n_dp, 2)
    near_side = swap_by(near, "dp", n_dp, 1)
    far_side = swap_by(far, "dp", n_dp, 1)
    both_side = swap_by(side, "dp", n_dp, 6)
    blocks = [block, side, near, near_side, far, far_side, both, both_side]
    return blocks, [g ^ k for k in range(n_dp)]


def in_order(blocks, places):
    stacked = jnp.zeros((len(blocks),) + blocks[0].shape, blocks[0].dtype)
    for place, block in zip(places, blocks):
        stacked = lax.dynamic_update_index_in_dim(stacked, block, place, 0)
    return stacked.reshape(-1, blocks[0].shape[1])


def make_body(n_dp, n_t):
    direct = n_dp == 8 and n_t == 4

    def body(hidden_in, norm_gain, w_in, conv_w, conv_b, w_dt_low, w_bc, w_dt, dt_bias, a_log,
             d_skip, w_out, conv_state, ssm_state, lengths, active_ids, active_count):
        slots, depth = hidden_in.shape
        rows = min(ACT_MAX, slots)
        share = depth // n_t
        width = conv_w.shape[1]
        block = w_in.shape[3]
        rank = w_dt_low.shape[1]
        count = a_log.shape[0]
        g = lax.axis_index("dp")
        t = lax.axis_index("tensor")

        def out(shape, dtype):
            return jax.ShapeDtypeStruct(shape, dtype)

        chosen, pick, spread, columns = pl.pallas_call(
            norm_kernel,
            out_shape=(
                out((rows, depth), BF16),
                out((rows, slots), BF16),
                out((slots, rows), BF16),
                out((slots, share), BF16),
            ),
            in_specs=[SMEM, SMEM, SMEM, VMEM, VMEM],
            out_specs=(VMEM,) * 4,
            name="norm",
        )(active_ids, active_count, t[None].astype(jnp.int32), hidden_in, norm_gain[None])
        if direct:
            blocks, places = gather_shared(chosen, g, t, n_dp, n_t)
            w_tied, blocks[TIE] = lax.optimization_barrier((w_in, blocks[TIE]))
            full = in_order(blocks, places)
        else:
            w_tied = w_in
            full = lax.all_gather(chosen, "dp", axis=0, tiled=True)
        branches = jnp.dot(full, w_tied.reshape(depth, 2 * block), preferred_element_type=F32)
        owned = lax.all_to_all(
            branches.astype(BF16), "dp", split_axis=0, concat_axis=0, tiled=True
        ).reshape(n_dp, rows, 2 * block)
        if block % 128 == 0:
            x_new = z_new = owned
        else:
            owned = jnp.transpose(owned.reshape(n_dp, rows, 2, block), (2, 1, 0, 3))
            x_new, z_new = owned[0].reshape(rows, width), owned[1].reshape(rows, width)
        known = lengths[:, None]
        past = jnp.transpose(conv_state, (1, 0, 2))
        packed, filtered, x_in, z_in = pl.pallas_call(
            filter_kernel,
            out_shape=(
                out((slots, rank + 2 * count), F32),
                out((slots, width), BF16),
                out((slots, width), BF16),
                out((slots, width), BF16),
            ),
            in_specs=[VMEM] * 9,
            out_specs=(VMEM,) * 4,
            name="filter",
        )(x_new, z_new, spread, known, past, conv_w, conv_b[None], w_dt_low, w_bc)
        active = jnp.sum(spread.astype(F32), axis=1, keepdims=True)
        if direct:
            sums = [packed] + [swap_by(packed, "tensor", n_t, m) for m in range(1, n_t)]
        else:
            sums = [lax.psum(packed, "tensor")]
        group, wide = 8, 2
        gated, states_next = pl.pallas_call(
            lambda *refs: state_kernel(*refs, parts=len(sums), group=group, wide=wide),
            out_shape=(out((rows, width), BF16), out((slots * count, width), F32)),
            in_specs=[VMEM] * (len(sums) + 9) + [HBM],
            out_specs=(VMEM, HBM),
            scratch_shapes=[
                pltpu.VMEM((width // 128, slots * count, 128), F32),
                pltpu.VMEM((width // 128, slots * count, 128), F32),
                pltpu.VMEM((slots, width), F32),
                pltpu.VMEM((slots, width), F32),
                pltpu.VMEM((count, slots, 128), F32),
                pltpu.VMEM((count, slots, 128), F32),
                pltpu.VMEM((count, width), F32),
                pltpu.VMEM((slots, width), F32),
                pltpu.SemaphoreType.DMA((slots // group, width // 128)),
                pltpu.SemaphoreType.DMA((slots // group, width // 128)),
            ],
            name="state",
        )(*sums, w_dt, dt_bias[None], a_log, d_skip[None], filtered, z_in, known, active, pick,
          ssm_state.reshape(slots * count, width))
        live = active[:, 0] > 0.5
        moved = jnp.concatenate([past[1:], x_in[None]], axis=0)
        conv_next = jnp.transpose(jnp.where(live[None, :, None], moved, past), (1, 0, 2))
        if direct:
            blocks, places = gather_own(gated, g, n_dp)
            partial = jnp.dot(in_order(blocks, places), w_out, preferred_element_type=F32)
            partial = partial.astype(BF16)
            base = 2 * (t ^ 2)
            pieces = [
                lax.dynamic_slice_in_dim(partial, (base ^ (2 * m)) * rows, 2 * rows, 0)
                for m in range(n_t)
            ]
            total = pieces[0].astype(F32)
            for m in range(1, n_t):
                total = total + swap_by(pieces[m], "tensor", n_t, m).astype(F32)
            total = total.astype(BF16)
            side = g % 2
            got = []
            for k in range(2):
                perm = []
                for gg in range(n_dp):
                    for tt in range(n_t):
                        dest = 2 * (tt ^ 2) + ((gg % 2) ^ k)
                        perm.append((gg * n_t + tt, dest * n_t + gg // 2))
                sent = lax.dynamic_slice_in_dim(total, (side ^ k) * rows, rows, 0)
                got.append(lax.ppermute(sent, ("dp", "tensor"), perm))
            first = jnp.where(side == 0, got[0], got[1])
            second = jnp.where(side == 0, got[1], got[0])
        else:
            gathered = lax.all_gather(gated, "dp", axis=0, tiled=True)
            partial = jnp.dot(gathered, w_out, preferred_element_type=F32).astype(BF16)
            by_sequence = lax.all_to_all(partial, "dp", split_axis=0, concat_axis=1, tiled=True)
            summed = lax.psum_scatter(by_sequence, "tensor", scatter_dimension=1, tiled=True)
            first, second = summed[:, : share // 2], summed[:, share // 2 :]
        mixed = pl.pallas_call(
            mix_kernel,
            out_shape=out((slots, share), BF16),
            in_specs=[VMEM] * 4,
            out_specs=VMEM,
            name="mix",
        )(spread, columns, first, second)
        return mixed, conv_next, states_next.reshape(slots, count, width)

    return body


def solution(mesh):
    in_specs = (
        P("dp", None),
        P(),
        P(None, None, "tensor", "dp"),
        P(None, "tensor"),
        P("tensor"),
        P("tensor", None),
        P(None, "tensor"),
        P(None, "tensor"),
        P("tensor"),
        P(None, "tensor"),
        P("tensor"),
        P("tensor", "dp"),
        P("dp", None, "tensor"),
        P("dp", None, "tensor"),
        P("dp"),
        P("dp", None),
        P("dp"),
    )
    out_specs = (P("dp", "tensor"), P("dp", None, "tensor"), P("dp", None, "tensor"))
    body = make_body(mesh.shape["dp"], mesh.shape["tensor"])
    return jax.shard_map(body, mesh=mesh, in_specs=in_specs, out_specs=out_specs, check_vma=False)
```

```python
import jax
import jax.numpy as jnp
from jax import lax
from jax.experimental import pallas as pl
from jax.experimental.pallas import tpu as pltpu
from jax.sharding import PartitionSpec as P


ACT_MAX = 24


F32 = jnp.float32
BF16 = jnp.bfloat16
VMEM = pl.BlockSpec(memory_space=pltpu.VMEM)
SMEM = pl.BlockSpec(memory_space=pltpu.SMEM)
HBM = pl.BlockSpec(memory_space=pltpu.HBM)


def near(values):
    return pltpu.with_memory_space_constraint(values, pltpu.VMEM)


def small(values):
    return pltpu.with_memory_space_constraint(values, pltpu.SMEM)


def away(values):
    return pltpu.with_memory_space_constraint(values, pltpu.HBM)


def limit(mebibytes):
    return pltpu.CompilerParams(vmem_limit_bytes=mebibytes * 1024 * 1024)


def rms_rows(values, epsilon):
    return values * lax.rsqrt(jnp.mean(values * values, axis=-1, keepdims=True) + epsilon)


def silu(values):
    return values / (1.0 + jnp.exp(-values))


def iota(shape, dim):
    return lax.broadcasted_iota(jnp.int32, shape, dim)


def norm_kernel(ids_hbm, hidden_hbm, gain_hbm, chosen, ids, hidden, gain, sems):
    pairs = ((ids_hbm, ids), (hidden_hbm, hidden), (gain_hbm, gain))
    copies = [pltpu.make_async_copy(a, b, sems.at[i]) for i, (a, b) in enumerate(pairs)]
    for copy in copies:
        copy.start()
    rows, slots = chosen.shape[0], hidden.shape[0]
    at = iota((rows, slots), 0), iota((rows, slots), 1)
    one_hot = jnp.zeros((rows, slots), F32)
    copies[0].wait()
    for j in range(rows):
        one_hot = jnp.where((at[0] == j) & (at[1] == ids[0, j]), 1.0, one_hot)
    for copy in copies[1:]:
        copy.wait()
    values = jnp.dot(one_hot.astype(BF16), hidden[...], preferred_element_type=F32)
    chosen[...] = (rms_rows(values, 1e-05) * gain[...]).astype(BF16)


def spread_matrix(ids, count, shape):
    at = iota(shape, 0), iota(shape, 1)
    live = jnp.zeros(shape, F32)
    for j in range(shape[1]):
        early = jnp.where(j < count[0], 1.0, 0.0)
        live = jnp.where((at[1] == j) & (at[0] == ids[0, j]), early, live)
    return live


def pick_matrix(ids, shape):
    at = iota(shape, 0), iota(shape, 1)
    one_hot = jnp.zeros(shape, F32)
    for j in range(shape[0]):
        one_hot = jnp.where((at[0] == j) & (at[1] == ids[0, j]), 1.0, one_hot)
    return one_hot


def prefetch_kernel(*refs, parts):
    sources, targets, sems = refs[:parts], refs[parts + 1 :][-parts - 1 : -1], refs[-1]
    extra = refs[parts + 1 : -parts - 1]
    copies = [
        pltpu.make_async_copy(a, b, sems.at[i]) for i, (a, b) in enumerate(zip(sources, targets))
    ]
    for copy in copies:
        copy.start()
    if extra:
        ids, count, spread, pick, live = extra
        matrix = spread_matrix(ids, count, spread.shape)
        spread[...] = matrix.astype(BF16)
        live[...] = jnp.sum(matrix, axis=1, keepdims=True)
        pick[...] = pick_matrix(ids, pick.shape).astype(BF16)
    for copy in copies:
        copy.wait()


def input_kernel(*refs, parts):
    own, place = refs[0][0], refs[1][0]
    blocks = refs[2 : 2 + parts]
    weights_hbm, branches, stacked, weights, sems = refs[2 + parts :]
    rows = blocks[0].shape[0]
    chunks = sems.shape[0]
    deep = weights.shape[0] // chunks
    pieces = [slice(i * deep, (i + 1) * deep) for i in range(chunks)]
    copies = [
        pltpu.make_async_copy(weights_hbm.at[at, :], weights.at[at, :], sems.at[i])
        for i, at in enumerate(pieces)
    ]
    for copy in copies:
        copy.start()
    for k, ref in enumerate(blocks):
        stacked[k * rows : (k + 1) * rows, :] = ref[...]
    result = None
    for copy, at in zip(copies, pieces):
        copy.wait()
        part = jnp.dot(stacked[:, at], weights[at, :], preferred_element_type=F32)
        result = part if result is None else result + part
    for k in range(parts):
        mask = jnp.where(place % 2 == 0, *SHARED_MASKS[k])
        branches[own ^ mask] = result[k * rows : (k + 1) * rows, :].astype(BF16)


def filter_kernel(spread, x_new, z_new, lengths, conv_state, conv_w, conv_b, w_dt_low, w_bc,
                  packed, filtered, x_in, z_in):
    taps = conv_w.shape[0]

    def branch(ref, first):
        if len(ref.shape) == 2:
            return ref[...]
        block = ref.shape[2] // 2
        parts = [ref[k, :, first * block : (first + 1) * block] for k in range(ref.shape[0])]
        return jnp.concatenate(parts, axis=1)

    def to_slots(values):
        return jnp.dot(spread[...], values, preferred_element_type=F32)

    x_slots = to_slots(branch(x_new, 0))
    x_in[...] = x_slots.astype(BF16)
    known = lengths[...]
    total = conv_w[taps - 1 : taps, :] * x_slots * (known >= 0).astype(F32)
    for k in range(taps - 1):
        usable = (known >= taps - 1 - k).astype(F32)
        total = total + conv_w[k : k + 1, :] * conv_state[k].astype(F32) * usable
    result = silu(total + conv_b[...]).astype(BF16)
    filtered[...] = result
    rank = w_dt_low.shape[1]
    packed[:, :rank] = jnp.dot(result, w_dt_low[...], preferred_element_type=F32)
    packed[:, rank:] = lax.dot_general(
        result, w_bc[...], (((1,), (1,)), ((), ())), preferred_element_type=F32
    )
    z_in[...] = to_slots(branch(z_new, 1)).astype(BF16)


def state_kernel(*refs, parts, group, wide):
    sums = refs[:parts]
    (pick, live, w_dt, dt_bias, a_log, d_skip, filtered, z_in, lengths, states,
     gated, states_next,
     result, step, drive, b_wide, c_wide, decay, pieces, out_sem) = refs[parts:]
    count = a_log.shape[0]
    slots, width = filtered.shape
    chunks = slots // group
    tiles = width // 128
    halves = count // 8
    span = group * halves * tiles * 8

    def save(k):
        piece = pl.ds(k * span, span)
        return pltpu.make_async_copy(result.at[piece], states_next.at[piece], out_sem.at[k])

    active = live[...] > 0.5
    total = sums[0][...]
    for other in sums[1:]:
        total = total + other[...]
    rank = w_dt.shape[0]
    low = rms_rows(total[:, :rank], 1e-06).astype(BF16)
    b_in = rms_rows(total[:, rank : rank + count], 1e-06)
    c_out = rms_rows(total[:, rank + count : rank + 2 * count], 1e-06)
    raw = jnp.dot(low, w_dt[...], preferred_element_type=F32) + dt_bias[...]
    size = jnp.maximum(raw, 0.0) + jnp.log1p(jnp.exp(-jnp.abs(raw)))
    fresh = lengths[...] > 0
    step[...] = jnp.where(active, jnp.where(fresh, size, 1e30), 0.0)
    drive[...] = jnp.where(active, size * filtered[...].astype(F32), 0.0)
    decay[...] = jnp.exp(a_log[...]) * -1.4426950408889634
    for n in range(count):
        at = pl.ds(n, slots, stride=count)
        b_wide[at, :] = jnp.broadcast_to(b_in[:, n : n + 1], (slots, 128))
        c_wide[at, :] = jnp.broadcast_to(c_out[:, n : n + 1], (slots, 128))
    for k in range(chunks):

        def column(i, carry):
            for u in range(wide):
                tile = i * wide + u
                lanes = pl.ds(pl.multiple_of(tile * 128, 128), 128)
                rates = [decay[h * 8 : h * 8 + 8, lanes] for h in range(halves)]
                for r in range(k * group, (k + 1) * group):
                    size = step[r : r + 1, lanes]
                    push = drive[r : r + 1, lanes]
                    y = None
                    for h in range(halves):
                        first = (r * halves + h) * tiles * 8 + tile * 8
                        at = pl.ds(pl.multiple_of(first, 8), 8)
                        own = slice(r * count + h * 8, r * count + h * 8 + 8)
                        new = jnp.exp2(size * rates[h]) * states[at, :] + push * b_wide[own, :]
                        result[at, :] = new
                        part = c_wide[own, :] * new
                        y = part if y is None else y + part
                    pieces[pl.ds(pl.multiple_of((tile * slots + r) * 8, 8), 8), :] = y
            return carry

        lax.fori_loop(0, tiles // wide, column, 0)
        save(k).start()
    outputs = []
    for tile in range(tiles):
        y = pieces[pl.ds(tile * slots * 8, slots, stride=8), :]
        for n in range(1, 8):
            y = y + pieces[pl.ds(tile * slots * 8 + n, slots, stride=8), :]
        outputs.append(y)
    filt = filtered[...].astype(F32)
    mixed = jnp.concatenate(outputs, axis=1) + d_skip[...] * filt
    mixed = (mixed * silu(z_in[...].astype(F32))).astype(BF16)
    gated[...] = jnp.dot(pick[...], mixed, preferred_element_type=F32).astype(BF16)
    for k in range(chunks):
        save(k).wait()


def mix_kernel(spread, columns, first, second, mixed):
    half = first.shape[1]
    matrix = spread[...]
    for i, ref in enumerate((first, second)):
        lanes = slice(i * half, (i + 1) * half)
        added = jnp.dot(matrix, ref[...], preferred_element_type=F32)
        mixed[:, lanes] = (columns[:, lanes].astype(F32) + added).astype(BF16)


def swap_by(values, axis, size, mask):
    return lax.ppermute(values, axis, [(i, i ^ mask) for i in range(size)])


def swap_by_core(values, n_dp, n_t, masks):
    perm = []
    for g in range(n_dp):
        for t in range(n_t):
            perm.append(((g ^ masks[t % 2]) * n_t + t, g * n_t + t))
    return lax.ppermute(values, ("dp", "tensor"), perm)


SHARED_MASKS = ((0, 0), (1, 1), (4, 2), (5, 3), (6, 7), (2, 4), (3, 5), (7, 6))


def gather_shared(block, weights, t, n_dp, n_t):
    even = t % 2 == 0
    side = swap_by_core(block, n_dp, n_t, (1, 1))
    far = swap_by_core(block, n_dp, n_t, (4, 2))
    far_side = swap_by_core(far, n_dp, n_t, (1, 1))
    last = swap_by_core(jnp.where(even, far, side), n_dp, n_t, (2, 6))
    weights, far = lax.optimization_barrier((weights, far))
    weights = weights.reshape(weights.shape[0], -1)
    weights, far_side, last = lax.optimization_barrier((weights, far_side, last))
    swapped = [swap_by(v, "tensor", n_t, 1) for v in (far, far_side, last)]
    return weights, [block, side, far, far_side, last] + swapped


def gather_own(block, g, n_dp):
    far, near, side = (swap_by(block, "dp", n_dp, m) for m in (4, 2, 1))
    both = swap_by(far, "dp", n_dp, 2)
    near_side = swap_by(near, "dp", n_dp, 1)
    far_side = swap_by(far, "dp", n_dp, 1)
    both_side = swap_by(side, "dp", n_dp, 6)
    blocks = [block, side, near, near_side, far, far_side, both, both_side]
    return blocks, [g ^ k for k in range(n_dp)]


def in_order(blocks, places):
    stacked = jnp.zeros((len(blocks),) + blocks[0].shape, blocks[0].dtype)
    for place, block in zip(places, blocks):
        stacked = lax.dynamic_update_index_in_dim(stacked, block, place, 0)
    return stacked.reshape(-1, blocks[0].shape[1])


def make_body(n_dp, n_t):
    direct = n_dp == 8 and n_t == 4

    def body(hidden_in, norm_gain, w_in, conv_w, conv_b, w_dt_low, w_bc, w_dt, dt_bias, a_log,
             d_skip, w_out, conv_state, ssm_state, lengths, active_ids, active_count):
        slots, depth = hidden_in.shape
        rows = min(ACT_MAX, slots)
        share = depth // n_t
        width = conv_w.shape[1]
        block = w_in.shape[3]
        rank = w_dt_low.shape[1]
        count = a_log.shape[0]
        g = lax.axis_index("dp")
        t = lax.axis_index("tensor")

        def out(shape, dtype):
            return jax.ShapeDtypeStruct(shape, dtype)

        def near_out(shape, dtype):
            return pltpu.VMEM(shape, dtype)

        own, place = small(g[None].astype(jnp.int32)), small(t[None].astype(jnp.int32))
        ids, held = small(active_ids), small(active_count)
        chosen = pl.pallas_call(
            norm_kernel,
            out_shape=near_out((rows, depth), BF16),
            in_specs=[HBM] * 3,
            out_specs=VMEM,
            scratch_shapes=[
                pltpu.SMEM(active_ids.shape, jnp.int32),
                pltpu.VMEM(hidden_in.shape, BF16),
                pltpu.VMEM((1, depth), F32),
                pltpu.SemaphoreType.DMA((3,)),
            ],
            compiler_params=limit(4),
            name="norm",
        )(away(active_ids), away(hidden_in), away(norm_gain[None]))

        def prefetch(values, after, *matrices):
            return pl.pallas_call(
                lambda *refs: prefetch_kernel(*refs, parts=len(values)),
                out_shape=matrices + tuple(near_out(v.shape, v.dtype) for v in values),
                in_specs=[HBM] * len(values)
                + [pl.BlockSpec(memory_space=pl.ANY)]
                + [SMEM] * (2 if matrices else 0),
                out_specs=(VMEM,) * (len(values) + len(matrices)),
                scratch_shapes=[pltpu.SemaphoreType.DMA((len(values),))],
                compiler_params=limit(1),
                name="prefetch",
            )(*[away(v) for v in values], after, *((ids, held) if matrices else ()))

        if direct:
            weights, blocks = gather_shared(chosen, w_in, t, n_dp, n_t)
            branches = pl.pallas_call(
                lambda *refs: input_kernel(*refs, parts=n_dp),
                out_shape=out((n_dp, rows, 2 * block), BF16),
                in_specs=[SMEM] * 2 + [VMEM] * n_dp + [HBM],
                out_specs=VMEM,
                scratch_shapes=[
                    pltpu.VMEM((n_dp * rows, depth), BF16),
                    pltpu.VMEM(weights.shape, BF16),
                    pltpu.SemaphoreType.DMA((4,)),
                ],
                compiler_params=limit(12),
                name="input",
            )(own, place, *[near(b) for b in blocks], away(weights))
        else:
            full = lax.all_gather(chosen, "dp", axis=0, tiled=True)
            branches = jnp.dot(full, w_in.reshape(depth, 2 * block), preferred_element_type=F32)
            branches = branches.astype(BF16).reshape(n_dp, rows, 2 * block)
        owned = lax.all_to_all(branches, "dp", split_axis=0, concat_axis=0, tiled=True)
        past = jnp.transpose(conv_state, (1, 0, 2))
        flat = slots * count * width // 128
        states = ssm_state.reshape(slots, count // 8, 8, width // 128, 128)
        states = jnp.transpose(states, (0, 1, 3, 2, 4)).reshape(flat, 128)
        spread, pick, live, past_n, conv_w_n, conv_b_n, w_dt_low_n, w_bc_n = prefetch(
            (past, conv_w, conv_b[None], w_dt_low, w_bc),
            branches,
            near_out((slots, rows), BF16),
            near_out((rows, slots), BF16),
            near_out((slots, 1), F32),
        )
        if block % 128 == 0:
            x_new = z_new = owned
        else:
            owned = jnp.transpose(owned.reshape(n_dp, rows, 2, block), (2, 1, 0, 3))
            x_new, z_new = owned[0].reshape(rows, width), owned[1].reshape(rows, width)
        known = lengths[:, None]
        packed, filtered, x_in, z_in = pl.pallas_call(
            filter_kernel,
            out_shape=(
                near_out((slots, rank + 2 * count), F32),
                near_out((slots, width), BF16),
                near_out((slots, width), BF16),
                near_out((slots, width), BF16),
            ),
            in_specs=[VMEM] * 9,
            out_specs=(VMEM,) * 4,
            compiler_params=limit(8),
            name="filter",
        )(near(spread), near(x_new), near(z_new), near(known), near(past_n), near(conv_w_n),
          near(conv_b_n), near(w_dt_low_n), near(w_bc_n))
        if direct:
            sums = [packed] + [swap_by(packed, "tensor", n_t, m) for m in range(1, n_t)]
        else:
            sums = [lax.psum(packed, "tensor")]
        w_dt_n, bias_n, a_log_n, skip_n, states_n = prefetch(
            (w_dt, dt_bias[None], a_log, d_skip[None], states), packed
        )
        group, wide = 8, 2
        gated, states_next = pl.pallas_call(
            lambda *refs: state_kernel(*refs, parts=len(sums), group=group, wide=wide),
            out_shape=(near_out((rows, width), BF16), out((flat, 128), F32)),
            in_specs=[VMEM] * (len(sums) + 10),
            out_specs=(VMEM, HBM),
            scratch_shapes=[
                pltpu.VMEM((flat, 128), F32),
                pltpu.VMEM((slots, width), F32),
                pltpu.VMEM((slots, width), F32),
                pltpu.VMEM((slots * count, 128), F32),
                pltpu.VMEM((slots * count, 128), F32),
                pltpu.VMEM((count, width), F32),
                pltpu.VMEM((slots * width // 16, 128), F32),
                pltpu.SemaphoreType.DMA((slots // group,)),
            ],
            compiler_params=limit(12),
            name="state",
        )(*[near(v) for v in sums], near(pick), near(live), near(w_dt_n), near(bias_n), near(a_log_n),
          near(skip_n), near(filtered), near(z_in), near(known), near(states_n))
        states_next = states_next.reshape(slots, count // 8, width // 128, 8, 128)
        states_next = jnp.transpose(states_next, (0, 1, 3, 2, 4))
        early = jnp.arange(slots, dtype=jnp.int32) < active_count[0]
        hits = (active_ids[0][:, None] == jnp.arange(slots, dtype=jnp.int32)[None, :]) & early[:, None]
        kept = jnp.any(hits, axis=0)
        moved = jnp.concatenate([past[1:], x_in[None]], axis=0)
        conv_next = jnp.transpose(jnp.where(kept[None, :, None], moved, past), (1, 0, 2))
        hidden_columns = lax.dynamic_slice_in_dim(hidden_in, t * share, share, 1)
        if direct:
            blocks, places = gather_own(gated, g, n_dp)
            w_out_n, columns = prefetch((w_out, hidden_columns), gated)
            partial = jnp.dot(in_order(blocks, places), w_out_n, preferred_element_type=F32)
            partial = partial.astype(BF16)
            base = 2 * (t ^ 2)
            pieces = [
                lax.dynamic_slice_in_dim(partial, (base ^ (2 * m)) * rows, 2 * rows, 0)
                for m in range(n_t)
            ]
            total = pieces[0].astype(F32)
            for m in range(1, n_t):
                total = total + swap_by(pieces[m], "tensor", n_t, m).astype(F32)
            total = total.astype(BF16)
            side = g % 2
            got = []
            for k in range(2):
                perm = []
                for gg in range(n_dp):
                    for tt in range(n_t):
                        dest = 2 * (tt ^ 2) + ((gg % 2) ^ k)
                        perm.append((gg * n_t + tt, dest * n_t + gg // 2))
                sent = lax.dynamic_slice_in_dim(total, (side ^ k) * rows, rows, 0)
                got.append(lax.ppermute(sent, ("dp", "tensor"), perm))
            first = jnp.where(side == 0, got[0], got[1])
            second = jnp.where(side == 0, got[1], got[0])
        else:
            _, columns = prefetch((w_out, hidden_columns), gated)
            gathered = lax.all_gather(gated, "dp", axis=0, tiled=True)
            partial = jnp.dot(gathered, w_out, preferred_element_type=F32).astype(BF16)
            by_sequence = lax.all_to_all(partial, "dp", split_axis=0, concat_axis=1, tiled=True)
            summed = lax.psum_scatter(by_sequence, "tensor", scatter_dimension=1, tiled=True)
            first, second = summed[:, : share // 2], summed[:, share // 2 :]
        mixed = pl.pallas_call(
            mix_kernel,
            out_shape=out((slots, share), BF16),
            in_specs=[VMEM] * 4,
            out_specs=VMEM,
            compiler_params=limit(2),
            name="mix",
        )(near(spread), near(columns), near(first), near(second))
        return mixed, conv_next, states_next.reshape(slots, count, width)

    return body


def solution(mesh):
    in_specs = (
        P("dp", None),
        P(),
        P(None, None, "tensor", "dp"),
        P(None, "tensor"),
        P("tensor"),
        P("tensor", None),
        P(None, "tensor"),
        P(None, "tensor"),
        P("tensor"),
        P(None, "tensor"),
        P("tensor"),
        P("tensor", "dp"),
        P("dp", None, "tensor"),
        P("dp", None, "tensor"),
        P("dp"),
        P("dp", None),
        P("dp"),
    )
    out_specs = (P("dp", "tensor"), P("dp", None, "tensor"), P("dp", None, "tensor"))
    inner = make_body(mesh.shape["dp"], mesh.shape["tensor"])

    return jax.shard_map(inner, mesh=mesh, in_specs=in_specs, out_specs=out_specs, check_vma=False)
```

```python
import jax
import jax.numpy as jnp
from jax import lax
from jax.experimental import pallas as pl
from jax.experimental.pallas import tpu as pltpu
from jax.sharding import PartitionSpec as P


ACT_MAX = 24


F32 = jnp.float32
BF16 = jnp.bfloat16
VMEM = pl.BlockSpec(memory_space=pltpu.VMEM)
SMEM = pl.BlockSpec(memory_space=pltpu.SMEM)
HBM = pl.BlockSpec(memory_space=pltpu.HBM)


def near(values):
    return pltpu.with_memory_space_constraint(values, pltpu.VMEM)


def small(values):
    return pltpu.with_memory_space_constraint(values, pltpu.SMEM)


def away(values):
    return pltpu.with_memory_space_constraint(values, pltpu.HBM)


def limit(mebibytes):
    return pltpu.CompilerParams(vmem_limit_bytes=mebibytes * 1024 * 1024)


def rms_rows(values, epsilon):
    return values * lax.rsqrt(jnp.mean(values * values, axis=-1, keepdims=True) + epsilon)


def silu(values):
    return values / (1.0 + jnp.exp(-values))


def iota(shape, dim):
    return lax.broadcasted_iota(jnp.int32, shape, dim)


def norm_kernel(ids_hbm, hidden_hbm, gain_hbm, chosen, ids, hidden, gain, sems):
    pairs = ((ids_hbm, ids), (hidden_hbm, hidden), (gain_hbm, gain))
    copies = [pltpu.make_async_copy(a, b, sems.at[i]) for i, (a, b) in enumerate(pairs)]
    for copy in copies:
        copy.start()
    rows, slots = chosen.shape[0], hidden.shape[0]
    at = iota((rows, slots), 0), iota((rows, slots), 1)
    one_hot = jnp.zeros((rows, slots), F32)
    copies[0].wait()
    for j in range(rows):
        one_hot = jnp.where((at[0] == j) & (at[1] == ids[0, j]), 1.0, one_hot)
    for copy in copies[1:]:
        copy.wait()
    values = jnp.dot(one_hot.astype(BF16), hidden[...], preferred_element_type=F32)
    chosen[...] = (rms_rows(values, 1e-05) * gain[...]).astype(BF16)


def spread_matrix(ids, count, shape):
    at = iota(shape, 0), iota(shape, 1)
    live = jnp.zeros(shape, F32)
    for j in range(shape[1]):
        early = jnp.where(j < count[0], 1.0, 0.0)
        live = jnp.where((at[1] == j) & (at[0] == ids[0, j]), early, live)
    return live


def pick_matrix(ids, shape):
    at = iota(shape, 0), iota(shape, 1)
    one_hot = jnp.zeros(shape, F32)
    for j in range(shape[0]):
        one_hot = jnp.where((at[0] == j) & (at[1] == ids[0, j]), 1.0, one_hot)
    return one_hot


def row_pieces(shape, dtype):
    size = jnp.dtype(dtype).itemsize
    for extent in shape:
        size *= extent
    cuts = 1
    while size // cuts > 2**18 and shape[0] % (32 * cuts) == 0:
        cuts *= 2
    rows = shape[0] // cuts
    return [pl.ds(i * rows, rows) for i in range(cuts)]


def prefetch_kernel(*refs, parts):
    sources, targets, sems = refs[:parts], refs[parts + 1 :][-parts - 1 : -1], refs[-1]
    extra = refs[parts + 1 : -parts - 1]
    copies = []
    for a, b in zip(sources, targets):
        for at in row_pieces(a.shape, a.dtype):
            copies.append(pltpu.make_async_copy(a.at[at], b.at[at], sems.at[len(copies)]))
    for copy in copies:
        copy.start()
    if extra:
        ids, count, spread, pick, live = extra
        matrix = spread_matrix(ids, count, spread.shape)
        spread[...] = matrix.astype(BF16)
        live[...] = jnp.sum(matrix, axis=1, keepdims=True)
        pick[...] = pick_matrix(ids, pick.shape).astype(BF16)
    for copy in copies:
        copy.wait()


def flush_kernel(source, target, sems):
    copies = [
        pltpu.make_async_copy(source.at[at], target.at[at], sems.at[i])
        for i, at in enumerate(row_pieces(source.shape, source.dtype))
    ]
    for copy in copies:
        copy.start()
    for copy in copies:
        copy.wait()


def input_kernel(*refs, parts):
    own, place = refs[0][0], refs[1][0]
    blocks = refs[2 : 2 + parts]
    upper, lower, branches, stacked = refs[2 + parts :]
    rows = blocks[0].shape[0]
    for k, ref in enumerate(blocks):
        stacked[k * rows : (k + 1) * rows, :] = ref[...]
    weights = jnp.concatenate([upper[...], lower[...]], axis=0)
    result = jnp.dot(stacked[...], weights, preferred_element_type=F32)
    for k in range(parts):
        mask = jnp.where(place % 2 == 0, *SHARED_MASKS[k])
        branches[own ^ mask] = result[k * rows : (k + 1) * rows, :].astype(BF16)


def filter_kernel(spread, x_new, z_new, lengths, conv_state, conv_w, conv_b, w_dt_low, w_bc,
                  packed, filtered, x_in, z_in):
    taps = conv_w.shape[0]

    def branch(ref, first):
        if len(ref.shape) == 2:
            return ref[...]
        block = ref.shape[2] // 2
        parts = [ref[k, :, first * block : (first + 1) * block] for k in range(ref.shape[0])]
        return jnp.concatenate(parts, axis=1)

    def to_slots(values):
        return jnp.dot(spread[...], values, preferred_element_type=F32)

    x_slots = to_slots(branch(x_new, 0))
    x_in[...] = x_slots.astype(BF16)
    known = lengths[...]
    total = conv_w[taps - 1 : taps, :] * x_slots * (known >= 0).astype(F32)
    for k in range(taps - 1):
        usable = (known >= taps - 1 - k).astype(F32)
        total = total + conv_w[k : k + 1, :] * conv_state[k].astype(F32) * usable
    result = silu(total + conv_b[...]).astype(BF16)
    filtered[...] = result
    rank = w_dt_low.shape[1]
    packed[:, :rank] = jnp.dot(result, w_dt_low[...], preferred_element_type=F32)
    packed[:, rank:] = lax.dot_general(
        result, w_bc[...], (((1,), (1,)), ((), ())), preferred_element_type=F32
    )
    z_in[...] = to_slots(branch(z_new, 1)).astype(BF16)


def state_kernel(*refs, parts, group, wide):
    sums = refs[:parts]
    (pick, live, w_dt, dt_bias, a_log, d_skip, filtered, z_in, lengths, states,
     gated, result,
     step, drive, b_wide, c_wide, decay, pieces) = refs[parts:]
    count = a_log.shape[0]
    slots, width = filtered.shape
    chunks = slots // group
    tiles = width // 128
    halves = count // 8
    active = live[...] > 0.5
    total = sums[0][...]
    for other in sums[1:]:
        total = total + other[...]
    rank = w_dt.shape[0]
    low = rms_rows(total[:, :rank], 1e-06).astype(BF16)
    b_in = rms_rows(total[:, rank : rank + count], 1e-06)
    c_out = rms_rows(total[:, rank + count : rank + 2 * count], 1e-06)
    raw = jnp.dot(low, w_dt[...], preferred_element_type=F32) + dt_bias[...]
    size = jnp.maximum(raw, 0.0) + jnp.log1p(jnp.exp(-jnp.abs(raw)))
    fresh = lengths[...] > 0
    step[...] = jnp.where(active, jnp.where(fresh, size, 1e30), 0.0)
    drive[...] = jnp.where(active, size * filtered[...].astype(F32), 0.0)
    decay[...] = jnp.exp(a_log[...]) * -1.4426950408889634
    for n in range(count):
        at = pl.ds(n, slots, stride=count)
        b_wide[at, :] = jnp.broadcast_to(b_in[:, n : n + 1], (slots, 128))
        c_wide[at, :] = jnp.broadcast_to(c_out[:, n : n + 1], (slots, 128))
    for k in range(chunks):

        def column(i, carry):
            for u in range(wide):
                tile = i * wide + u
                lanes = pl.ds(pl.multiple_of(tile * 128, 128), 128)
                rates = [decay[h * 8 : h * 8 + 8, lanes] for h in range(halves)]
                for r in range(k * group, (k + 1) * group):
                    size = step[r : r + 1, lanes]
                    push = drive[r : r + 1, lanes]
                    y = None
                    for h in range(halves):
                        first = (r * halves + h) * tiles * 8 + tile * 8
                        at = pl.ds(pl.multiple_of(first, 8), 8)
                        own = slice(r * count + h * 8, r * count + h * 8 + 8)
                        new = jnp.exp2(size * rates[h]) * states[at, :] + push * b_wide[own, :]
                        result[at, :] = new
                        part = c_wide[own, :] * new
                        y = part if y is None else y + part
                    pieces[pl.ds(pl.multiple_of((tile * slots + r) * 8, 8), 8), :] = y
            return carry

        lax.fori_loop(0, tiles // wide, column, 0)
    outputs = []
    for tile in range(tiles):
        y = pieces[pl.ds(tile * slots * 8, slots, stride=8), :]
        for n in range(1, 8):
            y = y + pieces[pl.ds(tile * slots * 8 + n, slots, stride=8), :]
        outputs.append(y)
    filt = filtered[...].astype(F32)
    mixed = jnp.concatenate(outputs, axis=1) + d_skip[...] * filt
    mixed = (mixed * silu(z_in[...].astype(F32))).astype(BF16)
    gated[...] = jnp.dot(pick[...], mixed, preferred_element_type=F32).astype(BF16)


def mix_kernel(spread, columns, first, second, mixed):
    half = first.shape[1]
    matrix = spread[...]
    for i, ref in enumerate((first, second)):
        lanes = slice(i * half, (i + 1) * half)
        added = jnp.dot(matrix, ref[...], preferred_element_type=F32)
        mixed[:, lanes] = (columns[:, lanes].astype(F32) + added).astype(BF16)


def swap_by(values, axis, size, mask):
    return lax.ppermute(values, axis, [(i, i ^ mask) for i in range(size)])


def swap_by_core(values, n_dp, n_t, masks):
    perm = []
    for g in range(n_dp):
        for t in range(n_t):
            perm.append(((g ^ masks[t % 2]) * n_t + t, g * n_t + t))
    return lax.ppermute(values, ("dp", "tensor"), perm)


SHARED_MASKS = ((0, 0), (1, 1), (4, 2), (5, 3), (6, 7), (2, 4), (3, 5), (7, 6))


def gather_shared(block, weights, fetch, t, n_dp, n_t):
    even = t % 2 == 0
    deep = weights.shape[0] // 2
    block, weights = lax.optimization_barrier((block, weights))
    upper = weights[:deep].reshape(deep, -1)
    side = swap_by_core(block, n_dp, n_t, (1, 1))
    far = swap_by_core(block, n_dp, n_t, (4, 2))
    far, upper, weights = lax.optimization_barrier((far, upper, weights))
    lower = weights[deep:].reshape(deep, -1)
    far_side = swap_by_core(far, n_dp, n_t, (1, 1))
    last = swap_by_core(jnp.where(even, far, side), n_dp, n_t, (2, 6))
    upper, lower = lax.optimization_barrier((upper, lower))
    upper, lower, far_side, last = lax.optimization_barrier(
        (fetch(upper), lower, far_side, last)
    )
    lower = fetch(lower)
    swapped = [swap_by(v, "tensor", n_t, 1) for v in (far, far_side, last)]
    return [upper, lower], [block, side, far, far_side, last] + swapped


def gather_own(block, g, n_dp):
    near, side = (swap_by(block, "dp", n_dp, m) for m in (2, 1))
    far = swap_by(block, "dp", n_dp, 4)
    side, far = lax.optimization_barrier((side, far))
    both = swap_by(far, "dp", n_dp, 2)
    near_side = swap_by(near, "dp", n_dp, 1)
    far_side = swap_by(far, "dp", n_dp, 1)
    both_side = swap_by(side, "dp", n_dp, 6)
    blocks = [block, side, near, near_side, far, far_side, both, both_side]
    return blocks, [g ^ k for k in range(n_dp)]


def in_order(blocks, places):
    stacked = jnp.zeros((len(blocks),) + blocks[0].shape, blocks[0].dtype)
    for place, block in zip(places, blocks):
        stacked = lax.dynamic_update_index_in_dim(stacked, block, place, 0)
    return stacked.reshape(-1, blocks[0].shape[1])


def make_body(n_dp, n_t):
    direct = n_dp == 8 and n_t == 4

    def body(hidden_in, norm_gain, w_in, conv_w, conv_b, w_dt_low, w_bc, w_dt, dt_bias, a_log,
             d_skip, w_out, conv_state, ssm_state, lengths, active_ids, active_count):
        slots, depth = hidden_in.shape
        rows = min(ACT_MAX, slots)
        share = depth // n_t
        width = conv_w.shape[1]
        block = w_in.shape[3]
        rank = w_dt_low.shape[1]
        count = a_log.shape[0]
        g = lax.axis_index("dp")
        t = lax.axis_index("tensor")

        def out(shape, dtype):
            return jax.ShapeDtypeStruct(shape, dtype)

        def near_out(shape, dtype):
            return pltpu.VMEM(shape, dtype)

        own, place = small(g[None].astype(jnp.int32)), small(t[None].astype(jnp.int32))
        ids, held = small(active_ids), small(active_count)
        chosen = pl.pallas_call(
            norm_kernel,
            out_shape=near_out((rows, depth), BF16),
            in_specs=[HBM] * 3,
            out_specs=VMEM,
            scratch_shapes=[
                pltpu.SMEM(active_ids.shape, jnp.int32),
                pltpu.VMEM(hidden_in.shape, BF16),
                pltpu.VMEM((1, depth), F32),
                pltpu.SemaphoreType.DMA((3,)),
            ],
            compiler_params=limit(4),
            name="norm",
        )(away(active_ids), away(hidden_in), away(norm_gain[None]))

        def prefetch(values, after, *matrices):
            return pl.pallas_call(
                lambda *refs: prefetch_kernel(*refs, parts=len(values)),
                out_shape=matrices + tuple(near_out(v.shape, v.dtype) for v in values),
                in_specs=[HBM] * len(values)
                + [pl.BlockSpec(memory_space=pl.ANY)]
                + [SMEM] * (2 if matrices else 0),
                out_specs=(VMEM,) * (len(values) + len(matrices)),
                scratch_shapes=[
                    pltpu.SemaphoreType.DMA(
                        (sum(len(row_pieces(v.shape, v.dtype)) for v in values),)
                    )
                ],
                compiler_params=limit(1),
                name="prefetch",
            )(*[away(v) for v in values], after, *((ids, held) if matrices else ()))

        if direct:
            def fetch(values):
                return prefetch((values,), chosen)[0]

            weights, blocks = gather_shared(chosen, w_in, fetch, t, n_dp, n_t)
            branches = pl.pallas_call(
                lambda *refs: input_kernel(*refs, parts=n_dp),
                out_shape=out((n_dp, rows, 2 * block), BF16),
                in_specs=[SMEM] * 2 + [VMEM] * (n_dp + 2),
                out_specs=VMEM,
                scratch_shapes=[
                    pltpu.VMEM((n_dp * rows, depth), BF16),
                ],
                compiler_params=limit(12),
                name="input",
            )(own, place, *[near(b) for b in blocks], *[near(w) for w in weights])
        else:
            full = lax.all_gather(chosen, "dp", axis=0, tiled=True)
            branches = jnp.dot(full, w_in.reshape(depth, 2 * block), preferred_element_type=F32)
            branches = branches.astype(BF16).reshape(n_dp, rows, 2 * block)
        owned = lax.all_to_all(branches, "dp", split_axis=0, concat_axis=0, tiled=True)
        past = jnp.transpose(conv_state, (1, 0, 2))
        flat = slots * count * width // 128
        states = ssm_state.reshape(slots, count // 8, 8, width // 128, 128)
        states = jnp.transpose(states, (0, 1, 3, 2, 4)).reshape(flat, 128)
        spread, pick, live, past_n, conv_w_n, conv_b_n, w_dt_low_n, w_bc_n = prefetch(
            (past, conv_w, conv_b[None], w_dt_low, w_bc),
            branches,
            near_out((slots, rows), BF16),
            near_out((rows, slots), BF16),
            near_out((slots, 1), F32),
        )
        if block % 128 == 0:
            x_new = z_new = owned
        else:
            owned = jnp.transpose(owned.reshape(n_dp, rows, 2, block), (2, 1, 0, 3))
            x_new, z_new = owned[0].reshape(rows, width), owned[1].reshape(rows, width)
        known = lengths[:, None]
        packed, filtered, x_in, z_in = pl.pallas_call(
            filter_kernel,
            out_shape=(
                near_out((slots, rank + 2 * count), F32),
                near_out((slots, width), BF16),
                near_out((slots, width), BF16),
                near_out((slots, width), BF16),
            ),
            in_specs=[VMEM] * 9,
            out_specs=(VMEM,) * 4,
            compiler_params=limit(8),
            name="filter",
        )(near(spread), near(x_new), near(z_new), near(known), near(past_n), near(conv_w_n),
          near(conv_b_n), near(w_dt_low_n), near(w_bc_n))
        if direct:
            sums = [packed] + [swap_by(packed, "tensor", n_t, m) for m in range(1, n_t)]
        else:
            sums = [lax.psum(packed, "tensor")]
        w_dt_n, bias_n, a_log_n, skip_n, states_n = prefetch(
            (w_dt, dt_bias[None], a_log, d_skip[None], states), packed
        )
        group, wide = 8, 2
        gated, states_next = pl.pallas_call(
            lambda *refs: state_kernel(*refs, parts=len(sums), group=group, wide=wide),
            out_shape=(near_out((rows, width), BF16), near_out((flat, 128), F32)),
            in_specs=[VMEM] * (len(sums) + 10),
            out_specs=(VMEM, VMEM),
            scratch_shapes=[
                pltpu.VMEM((slots, width), F32),
                pltpu.VMEM((slots, width), F32),
                pltpu.VMEM((slots * count, 128), F32),
                pltpu.VMEM((slots * count, 128), F32),
                pltpu.VMEM((count, width), F32),
                pltpu.VMEM((slots * width // 16, 128), F32),
            ],
            compiler_params=limit(8),
            name="state",
        )(*[near(v) for v in sums], near(pick), near(live), near(w_dt_n), near(bias_n), near(a_log_n),
          near(skip_n), near(filtered), near(z_in), near(known), near(states_n))
        states_next = pl.pallas_call(
            flush_kernel,
            out_shape=out((flat, 128), F32),
            in_specs=[VMEM],
            out_specs=HBM,
            scratch_shapes=[pltpu.SemaphoreType.DMA((len(row_pieces((flat, 128), F32)),))],
            compiler_params=limit(1),
            name="flush",
        )(near(states_next))
        states_next = states_next.reshape(slots, count // 8, width // 128, 8, 128)
        states_next = jnp.transpose(states_next, (0, 1, 3, 2, 4))
        early = jnp.arange(slots, dtype=jnp.int32) < active_count[0]
        hits = (active_ids[0][:, None] == jnp.arange(slots, dtype=jnp.int32)[None, :]) & early[:, None]
        kept = jnp.any(hits, axis=0)
        moved = jnp.concatenate([past[1:], x_in[None]], axis=0)
        conv_next = jnp.transpose(jnp.where(kept[None, :, None], moved, past), (1, 0, 2))
        hidden_columns = lax.dynamic_slice_in_dim(hidden_in, t * share, share, 1)
        if direct:
            blocks, places = gather_own(gated, g, n_dp)
            w_out_n, columns = prefetch((w_out, hidden_columns), gated)
            partial = jnp.dot(in_order(blocks, places), w_out_n, preferred_element_type=F32)
            partial = partial.astype(BF16)
            base = 2 * (t ^ 2)
            pieces = [
                lax.dynamic_slice_in_dim(partial, (base ^ (2 * m)) * rows, 2 * rows, 0)
                for m in range(n_t)
            ]
            total = pieces[0].astype(F32)
            for m in range(1, n_t):
                total = total + swap_by(pieces[m], "tensor", n_t, m).astype(F32)
            total = total.astype(BF16)
            side = g % 2
            got = []
            for k in range(2):
                perm = []
                for gg in range(n_dp):
                    for tt in range(n_t):
                        dest = 2 * (tt ^ 2) + ((gg % 2) ^ k)
                        perm.append((gg * n_t + tt, dest * n_t + gg // 2))
                sent = lax.dynamic_slice_in_dim(total, (side ^ k) * rows, rows, 0)
                got.append(lax.ppermute(sent, ("dp", "tensor"), perm))
            first = jnp.where(side == 0, got[0], got[1])
            second = jnp.where(side == 0, got[1], got[0])
        else:
            _, columns = prefetch((w_out, hidden_columns), gated)
            gathered = lax.all_gather(gated, "dp", axis=0, tiled=True)
            partial = jnp.dot(gathered, w_out, preferred_element_type=F32).astype(BF16)
            by_sequence = lax.all_to_all(partial, "dp", split_axis=0, concat_axis=1, tiled=True)
            summed = lax.psum_scatter(by_sequence, "tensor", scatter_dimension=1, tiled=True)
            first, second = summed[:, : share // 2], summed[:, share // 2 :]
        mixed = pl.pallas_call(
            mix_kernel,
            out_shape=out((slots, share), BF16),
            in_specs=[VMEM] * 4,
            out_specs=VMEM,
            compiler_params=limit(2),
            name="mix",
        )(near(spread), near(columns), near(first), near(second))
        return mixed, conv_next, states_next.reshape(slots, count, width)

    return body


def solution(mesh):
    in_specs = (
        P("dp", None),
        P(),
        P(None, None, "tensor", "dp"),
        P(None, "tensor"),
        P("tensor"),
        P("tensor", None),
        P(None, "tensor"),
        P(None, "tensor"),
        P("tensor"),
        P(None, "tensor"),
        P("tensor"),
        P("tensor", "dp"),
        P("dp", None, "tensor"),
        P("dp", None, "tensor"),
        P("dp"),
        P("dp", None),
        P("dp"),
    )
    out_specs = (P("dp", "tensor"), P("dp", None, "tensor"), P("dp", None, "tensor"))
    inner = make_body(mesh.shape["dp"], mesh.shape["tensor"])

    return jax.shard_map(inner, mesh=mesh, in_specs=in_specs, out_specs=out_specs, check_vma=False)
```

```python
import jax
import jax.numpy as jnp
from jax import lax
from jax.experimental import pallas as pl
from jax.experimental.pallas import tpu as pltpu
from jax.sharding import PartitionSpec as P


ACT_MAX = 24


F32 = jnp.float32
BF16 = jnp.bfloat16
VMEM = pl.BlockSpec(memory_space=pltpu.VMEM)
SMEM = pl.BlockSpec(memory_space=pltpu.SMEM)
HBM = pl.BlockSpec(memory_space=pltpu.HBM)


def near(values):
    return pltpu.with_memory_space_constraint(values, pltpu.VMEM)


def small(values):
    return pltpu.with_memory_space_constraint(values, pltpu.SMEM)


def away(values):
    return pltpu.with_memory_space_constraint(values, pltpu.HBM)


def limit(mebibytes):
    return pltpu.CompilerParams(vmem_limit_bytes=mebibytes * 1024 * 1024)


def rms_rows(values, epsilon):
    return values * lax.rsqrt(jnp.mean(values * values, axis=-1, keepdims=True) + epsilon)


def silu(values):
    return values / (1.0 + jnp.exp(-values))


def iota(shape, dim):
    return lax.broadcasted_iota(jnp.int32, shape, dim)


def norm_kernel(ids_hbm, hidden_hbm, gain_hbm, chosen, ids, hidden, gain, sems):
    pairs = ((ids_hbm, ids), (hidden_hbm, hidden), (gain_hbm, gain))
    copies = [pltpu.make_async_copy(a, b, sems.at[i]) for i, (a, b) in enumerate(pairs)]
    for copy in copies:
        copy.start()
    rows, slots = chosen.shape[0], hidden.shape[0]
    at = iota((rows, slots), 0), iota((rows, slots), 1)
    one_hot = jnp.zeros((rows, slots), F32)
    copies[0].wait()
    for j in range(rows):
        one_hot = jnp.where((at[0] == j) & (at[1] == ids[0, j]), 1.0, one_hot)
    for copy in copies[1:]:
        copy.wait()
    values = jnp.dot(one_hot.astype(BF16), hidden[...], preferred_element_type=F32)
    chosen[...] = (rms_rows(values, 1e-05) * gain[...]).astype(BF16)


def spread_matrix(ids, count, shape):
    at = iota(shape, 0), iota(shape, 1)
    live = jnp.zeros(shape, F32)
    for j in range(shape[1]):
        early = jnp.where(j < count[0], 1.0, 0.0)
        live = jnp.where((at[1] == j) & (at[0] == ids[0, j]), early, live)
    return live


def pick_matrix(ids, shape):
    at = iota(shape, 0), iota(shape, 1)
    one_hot = jnp.zeros(shape, F32)
    for j in range(shape[0]):
        one_hot = jnp.where((at[0] == j) & (at[1] == ids[0, j]), 1.0, one_hot)
    return one_hot


def row_pieces(shape, dtype):
    size = jnp.dtype(dtype).itemsize
    for extent in shape:
        size *= extent
    cuts = 1
    while size // cuts > 2**18 and shape[0] % (32 * cuts) == 0:
        cuts *= 2
    rows = shape[0] // cuts
    return [pl.ds(i * rows, rows) for i in range(cuts)]


def prefetch_kernel(*refs, parts):
    sources, targets, sems = refs[:parts], refs[parts + 1 :][-parts - 1 : -1], refs[-1]
    extra = refs[parts + 1 : -parts - 1]
    copies = []
    for a, b in zip(sources, targets):
        for at in row_pieces(a.shape, a.dtype):
            copies.append(pltpu.make_async_copy(a.at[at], b.at[at], sems.at[len(copies)]))
    for copy in copies:
        copy.start()
    if extra:
        ids, count, spread, pick, live = extra
        matrix = spread_matrix(ids, count, spread.shape)
        spread[...] = matrix.astype(BF16)
        live[...] = jnp.sum(matrix, axis=1, keepdims=True)
        pick[...] = pick_matrix(ids, pick.shape).astype(BF16)
    for copy in copies:
        copy.wait()


def flush_kernel(source, target, sems):
    copies = [
        pltpu.make_async_copy(source.at[at], target.at[at], sems.at[i])
        for i, at in enumerate(row_pieces(source.shape, source.dtype))
    ]
    for copy in copies:
        copy.start()
    for copy in copies:
        copy.wait()


def input_kernel(*refs, parts):
    own, place = refs[0][0], refs[1][0]
    blocks = refs[2 : 2 + parts]
    upper, lower, branches, stacked = refs[2 + parts :]
    rows = blocks[0].shape[0]
    for k, ref in enumerate(blocks):
        stacked[k * rows : (k + 1) * rows, :] = ref[...]
    weights = jnp.concatenate([upper[...], lower[...]], axis=0)
    result = jnp.dot(stacked[...], weights, preferred_element_type=F32)
    for k in range(parts):
        mask = jnp.where(place % 2 == 0, *SHARED_MASKS[k])
        branches[own ^ mask] = result[k * rows : (k + 1) * rows, :].astype(BF16)


def filter_kernel(spread, x_new, z_new, lengths, conv_state, conv_w, conv_b, w_dt_low, w_bc,
                  packed, sent, filtered, x_in, z_in):
    taps = conv_w.shape[0]

    def branch(ref, first):
        if len(ref.shape) == 2:
            return ref[...]
        block = ref.shape[2] // 2
        parts = [ref[k, :, first * block : (first + 1) * block] for k in range(ref.shape[0])]
        return jnp.concatenate(parts, axis=1)

    def to_slots(values):
        return jnp.dot(spread[...], values, preferred_element_type=F32)

    x_slots = to_slots(branch(x_new, 0))
    x_in[...] = x_slots.astype(BF16)
    known = lengths[...]
    total = conv_w[taps - 1 : taps, :] * x_slots * (known >= 0).astype(F32)
    for k in range(taps - 1):
        usable = (known >= taps - 1 - k).astype(F32)
        total = total + conv_w[k : k + 1, :] * conv_state[k].astype(F32) * usable
    result = silu(total + conv_b[...]).astype(BF16)
    filtered[...] = result
    rank = w_dt_low.shape[1]
    packed[:, :rank] = jnp.dot(result, w_dt_low[...], preferred_element_type=F32)
    packed[:, rank:] = lax.dot_general(
        result, w_bc[...], (((1,), (1,)), ((), ())), preferred_element_type=F32
    )
    sent[...] = packed[...].astype(BF16)
    z_in[...] = to_slots(branch(z_new, 1)).astype(BF16)


def state_kernel(*refs, parts, group, wide):
    sums = refs[:parts]
    (pick, live, w_dt, dt_bias, a_log, d_skip, filtered, z_in, lengths, states,
     gated, result,
     step, drive, b_wide, c_wide, decay, pieces) = refs[parts:]
    count = a_log.shape[0]
    slots, width = filtered.shape
    chunks = slots // group
    tiles = width // 128
    halves = count // 8
    active = live[...] > 0.5
    total = sums[0][...]
    for other in sums[1:]:
        total = total + other[...].astype(F32)
    rank = w_dt.shape[0]
    low = rms_rows(total[:, :rank], 1e-06).astype(BF16)
    b_in = rms_rows(total[:, rank : rank + count], 1e-06)
    c_out = rms_rows(total[:, rank + count : rank + 2 * count], 1e-06)
    raw = jnp.dot(low, w_dt[...], preferred_element_type=F32) + dt_bias[...]
    size = jnp.maximum(raw, 0.0) + jnp.log1p(jnp.exp(-jnp.abs(raw)))
    fresh = lengths[...] > 0
    step[...] = jnp.where(active, jnp.where(fresh, size, 1e30), 0.0)
    drive[...] = jnp.where(active, size * filtered[...].astype(F32), 0.0)
    decay[...] = jnp.exp(a_log[...]) * -1.4426950408889634
    for n in range(count):
        at = pl.ds(n, slots, stride=count)
        b_wide[at, :] = jnp.broadcast_to(b_in[:, n : n + 1], (slots, 128))
        c_wide[at, :] = jnp.broadcast_to(c_out[:, n : n + 1], (slots, 128))
    for k in range(chunks):

        def column(i, carry):
            for u in range(wide):
                tile = i * wide + u
                lanes = pl.ds(pl.multiple_of(tile * 128, 128), 128)
                rates = [decay[h * 8 : h * 8 + 8, lanes] for h in range(halves)]
                for r in range(k * group, (k + 1) * group):
                    size = step[r : r + 1, lanes]
                    push = drive[r : r + 1, lanes]
                    y = None
                    for h in range(halves):
                        first = (r * halves + h) * tiles * 8 + tile * 8
                        at = pl.ds(pl.multiple_of(first, 8), 8)
                        own = slice(r * count + h * 8, r * count + h * 8 + 8)
                        new = jnp.exp2(size * rates[h]) * states[at, :] + push * b_wide[own, :]
                        result[at, :] = new
                        part = c_wide[own, :] * new
                        y = part if y is None else y + part
                    pieces[pl.ds(pl.multiple_of((tile * slots + r) * 8, 8), 8), :] = y
            return carry

        lax.fori_loop(0, tiles // wide, column, 0)
    outputs = []
    for tile in range(tiles):
        y = pieces[pl.ds(tile * slots * 8, slots, stride=8), :]
        for n in range(1, 8):
            y = y + pieces[pl.ds(tile * slots * 8 + n, slots, stride=8), :]
        outputs.append(y)
    filt = filtered[...].astype(F32)
    mixed = jnp.concatenate(outputs, axis=1) + d_skip[...] * filt
    mixed = (mixed * silu(z_in[...].astype(F32))).astype(BF16)
    gated[...] = jnp.dot(pick[...], mixed, preferred_element_type=F32).astype(BF16)


def mix_kernel(spread, columns, first, second, mixed):
    half = first.shape[1]
    matrix = spread[...]
    for i, ref in enumerate((first, second)):
        lanes = slice(i * half, (i + 1) * half)
        added = jnp.dot(matrix, ref[...], preferred_element_type=F32)
        mixed[:, lanes] = (columns[:, lanes].astype(F32) + added).astype(BF16)


def swap_by(values, axis, size, mask):
    return lax.ppermute(values, axis, [(i, i ^ mask) for i in range(size)])


def swap_by_core(values, n_dp, n_t, masks):
    perm = []
    for g in range(n_dp):
        for t in range(n_t):
            perm.append(((g ^ masks[t % 2]) * n_t + t, g * n_t + t))
    return lax.ppermute(values, ("dp", "tensor"), perm)


SHARED_MASKS = ((0, 0), (1, 1), (4, 2), (5, 3), (6, 7), (2, 4), (3, 5), (7, 6))


def gather_shared(block, weights, fetch, t, n_dp, n_t):
    even = t % 2 == 0
    deep = weights.shape[0] * 7 // 16
    block, weights = lax.optimization_barrier((block, weights))
    upper = weights[:deep].reshape(deep, -1)
    side = swap_by_core(block, n_dp, n_t, (1, 1))
    far = swap_by_core(block, n_dp, n_t, (4, 2))
    far, upper, weights = lax.optimization_barrier((far, upper, weights))
    lower = weights[deep:].reshape(weights.shape[0] - deep, -1)
    far_side = swap_by_core(far, n_dp, n_t, (1, 1))
    last = swap_by_core(jnp.where(even, far, side), n_dp, n_t, (2, 6))
    upper, lower = lax.optimization_barrier((upper, lower))
    upper, lower, far_side, last = lax.optimization_barrier(
        (fetch(upper), lower, far_side, last)
    )
    lower = fetch(lower)
    swapped = [swap_by(v, "tensor", n_t, 1) for v in (far, far_side, last)]
    return [upper, lower], [block, side, far, far_side, last] + swapped


def gather_own(block, g, n_dp):
    far = swap_by(block, "dp", n_dp, 4)
    near = swap_by(block, "dp", n_dp, 2)
    side = swap_by(block, "dp", n_dp, 1)
    side, far = lax.optimization_barrier((side, far))
    both = swap_by(far, "dp", n_dp, 2)
    near_side = swap_by(near, "dp", n_dp, 1)
    far_side = swap_by(far, "dp", n_dp, 1)
    both_side = swap_by(side, "dp", n_dp, 6)
    blocks = [block, side, near, near_side, far, far_side, both, both_side]
    return blocks, [g ^ k for k in range(n_dp)]


def in_order(blocks, places):
    stacked = jnp.zeros((len(blocks),) + blocks[0].shape, blocks[0].dtype)
    for place, block in zip(places, blocks):
        stacked = lax.dynamic_update_index_in_dim(stacked, block, place, 0)
    return stacked.reshape(-1, blocks[0].shape[1])


def make_body(n_dp, n_t):
    direct = n_dp == 8 and n_t == 4

    def body(hidden_in, norm_gain, w_in, conv_w, conv_b, w_dt_low, w_bc, w_dt, dt_bias, a_log,
             d_skip, w_out, conv_state, ssm_state, lengths, active_ids, active_count):
        slots, depth = hidden_in.shape
        rows = min(ACT_MAX, slots)
        share = depth // n_t
        width = conv_w.shape[1]
        block = w_in.shape[3]
        rank = w_dt_low.shape[1]
        count = a_log.shape[0]
        g = lax.axis_index("dp")
        t = lax.axis_index("tensor")

        def out(shape, dtype):
            return jax.ShapeDtypeStruct(shape, dtype)

        def near_out(shape, dtype):
            return pltpu.VMEM(shape, dtype)

        own, place = small(g[None].astype(jnp.int32)), small(t[None].astype(jnp.int32))
        ids, held = small(active_ids), small(active_count)
        chosen = pl.pallas_call(
            norm_kernel,
            out_shape=near_out((rows, depth), BF16),
            in_specs=[HBM] * 3,
            out_specs=VMEM,
            scratch_shapes=[
                pltpu.SMEM(active_ids.shape, jnp.int32),
                pltpu.VMEM(hidden_in.shape, BF16),
                pltpu.VMEM((1, depth), F32),
                pltpu.SemaphoreType.DMA((3,)),
            ],
            compiler_params=limit(4),
            name="norm",
        )(away(active_ids), away(hidden_in), away(norm_gain[None]))

        def prefetch(values, after, *matrices):
            return pl.pallas_call(
                lambda *refs: prefetch_kernel(*refs, parts=len(values)),
                out_shape=matrices + tuple(near_out(v.shape, v.dtype) for v in values),
                in_specs=[HBM] * len(values)
                + [pl.BlockSpec(memory_space=pl.ANY)]
                + [SMEM] * (2 if matrices else 0),
                out_specs=(VMEM,) * (len(values) + len(matrices)),
                scratch_shapes=[
                    pltpu.SemaphoreType.DMA(
                        (sum(len(row_pieces(v.shape, v.dtype)) for v in values),)
                    )
                ],
                compiler_params=limit(1),
                name="prefetch",
            )(*[away(v) for v in values], after, *((ids, held) if matrices else ()))

        if direct:
            def fetch(values):
                return prefetch((values,), chosen)[0]

            weights, blocks = gather_shared(chosen, w_in, fetch, t, n_dp, n_t)
            branches = pl.pallas_call(
                lambda *refs: input_kernel(*refs, parts=n_dp),
                out_shape=out((n_dp, rows, 2 * block), BF16),
                in_specs=[SMEM] * 2 + [VMEM] * (n_dp + 2),
                out_specs=VMEM,
                scratch_shapes=[
                    pltpu.VMEM((n_dp * rows, depth), BF16),
                ],
                compiler_params=limit(12),
                name="input",
            )(own, place, *[near(b) for b in blocks], *[near(w) for w in weights])
        else:
            full = lax.all_gather(chosen, "dp", axis=0, tiled=True)
            branches = jnp.dot(full, w_in.reshape(depth, 2 * block), preferred_element_type=F32)
            branches = branches.astype(BF16).reshape(n_dp, rows, 2 * block)
        owned = lax.all_to_all(branches, "dp", split_axis=0, concat_axis=0, tiled=True)
        past = jnp.transpose(conv_state, (1, 0, 2))
        flat = slots * count * width // 128
        states = ssm_state.reshape(slots, count // 8, 8, width // 128, 128)
        states = jnp.transpose(states, (0, 1, 3, 2, 4)).reshape(flat, 128)
        (
            spread, pick, live, past_n, conv_w_n, conv_b_n, w_dt_low_n, w_bc_n, w_dt_n, bias_n,
            a_log_n, skip_n,
        ) = prefetch(
            (past, conv_w, conv_b[None], w_dt_low, w_bc, w_dt, dt_bias[None], a_log, d_skip[None]),
            branches,
            near_out((slots, rows), BF16),
            near_out((rows, slots), BF16),
            near_out((slots, 1), F32),
        )
        if block % 128 == 0:
            x_new = z_new = owned
        else:
            owned = jnp.transpose(owned.reshape(n_dp, rows, 2, block), (2, 1, 0, 3))
            x_new, z_new = owned[0].reshape(rows, width), owned[1].reshape(rows, width)
        known = lengths[:, None]
        packed, sent, filtered, x_in, z_in = pl.pallas_call(
            filter_kernel,
            out_shape=(
                near_out((slots, rank + 2 * count), F32),
                near_out((slots, rank + 2 * count), BF16),
                near_out((slots, width), BF16),
                near_out((slots, width), BF16),
                near_out((slots, width), BF16),
            ),
            in_specs=[VMEM] * 9,
            out_specs=(VMEM,) * 5,
            compiler_params=limit(8),
            name="filter",
        )(near(spread), near(x_new), near(z_new), near(known), near(past_n), near(conv_w_n),
          near(conv_b_n), near(w_dt_low_n), near(w_bc_n))
        if direct:
            sums = [packed] + [swap_by(sent, "tensor", n_t, m) for m in range(1, n_t)]
        else:
            sums = [lax.psum(packed, "tensor")]
        (states_n,) = prefetch((states,), packed)
        group, wide = 8, 4
        gated, states_next = pl.pallas_call(
            lambda *refs: state_kernel(*refs, parts=len(sums), group=group, wide=wide),
            out_shape=(near_out((rows, width), BF16), near_out((flat, 128), F32)),
            in_specs=[VMEM] * (len(sums) + 10),
            out_specs=(VMEM, VMEM),
            scratch_shapes=[
                pltpu.VMEM((slots, width), F32),
                pltpu.VMEM((slots, width), F32),
                pltpu.VMEM((slots * count, 128), F32),
                pltpu.VMEM((slots * count, 128), F32),
                pltpu.VMEM((count, width), F32),
                pltpu.VMEM((slots * width // 16, 128), F32),
            ],
            compiler_params=limit(8),
            name="state",
        )(*[near(v) for v in sums], near(pick), near(live), near(w_dt_n), near(bias_n), near(a_log_n),
          near(skip_n), near(filtered), near(z_in), near(known), near(states_n))
        states_next = pl.pallas_call(
            flush_kernel,
            out_shape=out((flat, 128), F32),
            in_specs=[VMEM],
            out_specs=HBM,
            scratch_shapes=[pltpu.SemaphoreType.DMA((len(row_pieces((flat, 128), F32)),))],
            compiler_params=limit(1),
            name="flush",
        )(near(states_next))
        states_next = states_next.reshape(slots, count // 8, width // 128, 8, 128)
        states_next = jnp.transpose(states_next, (0, 1, 3, 2, 4))
        early = jnp.arange(slots, dtype=jnp.int32) < active_count[0]
        hits = (active_ids[0][:, None] == jnp.arange(slots, dtype=jnp.int32)[None, :]) & early[:, None]
        kept = jnp.any(hits, axis=0)
        moved = jnp.concatenate([past[1:], x_in[None]], axis=0)
        conv_next = jnp.transpose(jnp.where(kept[None, :, None], moved, past), (1, 0, 2))
        hidden_columns = lax.dynamic_slice_in_dim(hidden_in, t * share, share, 1)
        if direct:
            blocks, places = gather_own(gated, g, n_dp)
            w_out_n, columns = prefetch((w_out, hidden_columns), gated)
            partial = jnp.dot(in_order(blocks, places), w_out_n, preferred_element_type=F32)
            partial = partial.astype(BF16)
            base = 2 * (t ^ 2)
            pieces = [
                lax.dynamic_slice_in_dim(partial, (base ^ (2 * m)) * rows, 2 * rows, 0)
                for m in range(n_t)
            ]
            total = pieces[0].astype(F32)
            for m in range(1, n_t):
                total = total + swap_by(pieces[m], "tensor", n_t, m).astype(F32)
            total = total.astype(BF16)
            side = g % 2
            got = []
            for k in range(2):
                perm = []
                for gg in range(n_dp):
                    for tt in range(n_t):
                        dest = 2 * (tt ^ 2) + ((gg % 2) ^ k)
                        perm.append((gg * n_t + tt, dest * n_t + gg // 2))
                sent = lax.dynamic_slice_in_dim(total, (side ^ k) * rows, rows, 0)
                got.append(lax.ppermute(sent, ("dp", "tensor"), perm))
            first = jnp.where(side == 0, got[0], got[1])
            second = jnp.where(side == 0, got[1], got[0])
        else:
            _, columns = prefetch((w_out, hidden_columns), gated)
            gathered = lax.all_gather(gated, "dp", axis=0, tiled=True)
            partial = jnp.dot(gathered, w_out, preferred_element_type=F32).astype(BF16)
            by_sequence = lax.all_to_all(partial, "dp", split_axis=0, concat_axis=1, tiled=True)
            summed = lax.psum_scatter(by_sequence, "tensor", scatter_dimension=1, tiled=True)
            first, second = summed[:, : share // 2], summed[:, share // 2 :]
        mixed = pl.pallas_call(
            mix_kernel,
            out_shape=out((slots, share), BF16),
            in_specs=[VMEM] * 4,
            out_specs=VMEM,
            compiler_params=limit(2),
            name="mix",
        )(near(spread), near(columns), near(first), near(second))
        return mixed, conv_next, states_next.reshape(slots, count, width)

    return body


def solution(mesh):
    in_specs = (
        P("dp", None),
        P(),
        P(None, None, "tensor", "dp"),
        P(None, "tensor"),
        P("tensor"),
        P("tensor", None),
        P(None, "tensor"),
        P(None, "tensor"),
        P("tensor"),
        P(None, "tensor"),
        P("tensor"),
        P("tensor", "dp"),
        P("dp", None, "tensor"),
        P("dp", None, "tensor"),
        P("dp"),
        P("dp", None),
        P("dp"),
    )
    out_specs = (P("dp", "tensor"), P("dp", None, "tensor"), P("dp", None, "tensor"))
    inner = make_body(mesh.shape["dp"], mesh.shape["tensor"])

    return jax.shard_map(inner, mesh=mesh, in_specs=in_specs, out_specs=out_specs, check_vma=False)
```
